128 devices in a mesh: seq: 32 (over x, z, core), head: 4 (over y).
Axes of the slice: x: 4, y: 4, z: 4, core: 2. Of those that a mesh axis runs over, the one named last changes fastest.
Arguments:
- queries: bfloat16 [24576, 8192], P('seq', 'head'), may hold values from -6 to 6
- key_rows: bfloat16 [24576, 8192], P('seq', 'head'), may hold values from -0.5 to 0.5
- value_rows: bfloat16 [24576, 8192], P('seq', 'head'), may hold values from -130 to 130
- log_decay: float32 [64, 24576], P('head', 'seq'), may hold values from -1 to 0
- norm_gain: float32 [8192], P('head'), may hold values from 0.1 to 1.9
- grad_out: bfloat16 [24576, 8192], P('seq', 'head'), may hold values from -13 to 13
Outputs:
- output: bfloat16 [24576, 8192], P('seq', 'head')
- grad_queries: bfloat16 [24576, 8192], P('seq', 'head')
- grad_keys: bfloat16 [24576, 8192], P('seq', 'head')
- grad_values: bfloat16 [24576, 8192], P('seq', 'head')
- grad_gain: float32 [8192], P('head')
The draws below stay inside these ranges and needn't reach their ends.
All inputs are finite; a program needn't handle non-finite values.
Results may differ from the reference program's by a relative error of at most 0.01.
Values sent between devices are 32-bit elements; how exact they have to be, the bound alone decides.
No kernel may reach another device: no remote copies, remote signals or barrier semaphores. Data moves between devices by JAX's collectives and lax.ppermute only.
A program may use at most 192 MiB of HBM per device.

```python
import jax
import jax.numpy as jnp
from jax import lax

HEADS = 64
DH = 128
TOK_DEV = 768
SEQUENCE_TOKENS = 24576
HD = 8192


def draw_log_decay(key, part):
    sample_sequences = jax.random.split(key, 6)
    token_position = jnp.arange(SEQUENCE_TOKENS)
    fast_share = 0.5
    picked = jax.random.uniform(sample_sequences[0], (HEADS, 1), dtype=jnp.float32)
    fast_rate = jnp.exp(jax.random.uniform(sample_sequences[1], (HEADS, 1), dtype=jnp.float32, minval=jnp.log(1.0 / 50.0), maxval=jnp.log(1.0 / 30.0)))
    slow_rate = 0.6 / SEQUENCE_TOKENS
    baseline_decay_rate = jnp.where(picked < fast_share, fast_rate, slow_rate)
    block_count = SEQUENCE_TOKENS // TOK_DEV
    block_multiplier = jnp.exp(jax.random.uniform(sample_sequences[2], (HEADS, block_count), dtype=jnp.float32, minval=jnp.log(0.5), maxval=jnp.log(2.0)))
    block_multiplier = jnp.repeat(block_multiplier, TOK_DEV, axis=1, total_repeat_length=SEQUENCE_TOKENS)
    jitter_amplitude = jax.random.uniform(sample_sequences[3], (HEADS, SEQUENCE_TOKENS), dtype=jnp.float32, minval=0.5, maxval=1.5)
    spike_locations = jax.random.randint(sample_sequences[4], (3,), 0, SEQUENCE_TOKENS)
    spike_magnitude = jax.random.uniform(sample_sequences[5], (HEADS, 3), dtype=jnp.float32, minval=0.22, maxval=0.69)
    decay_spikes = jnp.sum(jnp.where(token_position[None, :, None] == spike_locations[None, None, :], spike_magnitude[:, None, :], 0.0), axis=2)
    return (-(baseline_decay_rate * block_multiplier * jitter_amplitude + decay_spikes)).astype(jnp.float32)


def draw_value_rows(key, part):
    sample_sequences = jax.random.split(key, 3)
    head_number = (jnp.arange(HD) // DH).astype(jnp.float32)
    head_scale = 1.0 + 2.0 * head_number / max(HEADS - 1, 1)
    base = jnp.clip(jax.random.normal(sample_sequences[0], (SEQUENCE_TOKENS, HD), dtype=jnp.float32), -4.0, 4.0)
    row_scale = jnp.exp(jax.random.uniform(sample_sequences[2], (SEQUENCE_TOKENS, 1), dtype=jnp.float32, minval=0.0, maxval=jnp.log(10.0)))
    return (base * head_scale[None, :] * row_scale).astype(jnp.bfloat16)


def draw_grad_out(key, part):
    sample_sequences = jax.random.split(key, 1)
    ramp = 1.0 + 2.0 * jnp.arange(SEQUENCE_TOKENS).astype(jnp.float32) / (SEQUENCE_TOKENS - 1)
    base = jnp.clip(jax.random.normal(sample_sequences[0], (SEQUENCE_TOKENS, HD), dtype=jnp.float32), -4.0, 4.0)
    return (base * ramp[:, None]).astype(jnp.bfloat16)


def level_of(rng, dims, cuts, least, largest):
    def one(axis_at, parts):
        draws = jax.random.uniform(jax.random.fold_in(jax.random.fold_in(rng, 6), axis_at), (parts,), jnp.float32, least / len(cuts), largest / len(cuts))
        return jnp.repeat(jnp.exp(draws), dims[axis_at] // parts).reshape((-1,) + (1,) * (len(dims) - axis_at - 1))

    factor_of = one(*cuts[0])
    for cut in cuts[1:]:
        factor_of = factor_of * one(*cut)
    return factor_of


def normal_values(rng, extent, width, limit, cuts=(), held_as=jnp.bfloat16):
    result = jax.random.normal(rng, extent, jnp.float32) * width
    if len(cuts) > 0:
        result = level_of(rng, extent, cuts, -0.22, 0.18) * result
    return jnp.clip(result, min=-limit, max=limit).astype(held_as)


def setup_inputs(seed: int = 0) -> dict:
    arg_keys = jax.random.split(jax.random.key(seed), 7)
    queries = normal_values(arg_keys[0], (SEQUENCE_TOKENS, HD), 1.0, 6.0, ((0, 32), (1, 4)))
    key_rows = normal_values(arg_keys[1], (SEQUENCE_TOKENS, HD), DH ** -0.5, 0.5, ((0, 32), (1, 4)))
    value_rows = draw_value_rows(jax.random.fold_in(arg_keys[6], 71), 0)
    log_decay = draw_log_decay(jax.random.fold_in(arg_keys[6], 71), 0)
    norm_gain = jnp.clip(1.0 + 0.18 * jax.random.normal(arg_keys[4], (HD,), jnp.float32), 0.1, 1.9)
    grad_out = draw_grad_out(jax.random.fold_in(arg_keys[6], 71), 0)
    return dict(queries=queries, key_rows=key_rows, value_rows=value_rows, log_decay=log_decay, norm_gain=norm_gain, grad_out=grad_out)


EPSILON = 1e-06

def exact_product(form, left, right):
    return jnp.einsum(form, left.astype(jnp.float32), right.astype(jnp.float32), precision=lax.Precision.HIGHEST)

def plain_product(form, left, right):
    return jnp.einsum(form, left.astype(jnp.float32), right.astype(jnp.float32))

def causal_decay(cumulative):
    length = cumulative.shape[-1]
    below_diag = jnp.arange(length)[:, None] >= jnp.arange(length)[None, :]
    spread = cumulative[..., :, None] - cumulative[..., None, :]
    return jnp.where(below_diag, jnp.exp(jnp.where(below_diag, spread, 0.0)), 0.0)

def split_heads(matrix):
    return matrix.reshape(matrix.shape[0], HEADS, DH).transpose(1, 0, 2)

def merge_heads(tensor):
    return tensor.transpose(1, 0, 2).reshape(tensor.shape[1], HD)

def attend(q_heads, k_heads, v_heads, cumulative, state):
    decay_mask = causal_decay(cumulative)
    scores = plain_product('htd,hsd->hts', q_heads, k_heads)
    weights = (scores * decay_mask).astype(jnp.bfloat16)
    attended = plain_product('hts,hsd->htd', weights, v_heads)
    attended = attended + jnp.exp(cumulative)[..., None] * exact_product('htd,hde->hte', q_heads, state)
    return (attended, weights, decay_mask)

def normalize(attended, grad_rows, norm_gain):
    mixed = merge_heads(attended)
    inverse = lax.rsqrt(lax.optimization_barrier(jnp.mean(mixed * mixed, axis=1)) + EPSILON)
    normed = mixed * inverse[:, None]
    scaled = grad_rows.astype(jnp.float32) * norm_gain[None, :]
    center = lax.optimization_barrier(jnp.mean(scaled * normed, axis=1))
    grad_attended = (inverse[:, None] * (scaled - normed * center[:, None])).astype(jnp.bfloat16)
    return (normed, split_heads(grad_attended))

def reference(queries, key_rows, value_rows, log_decay, norm_gain, grad_out):
    blocks = SEQUENCE_TOKENS // TOK_DEV

    def tile(matrix):
        return matrix.reshape(blocks, TOK_DEV, HEADS, DH).transpose(0, 2, 1, 3)
    q_all = tile(queries)
    k_all = tile(key_rows)
    v_all = tile(value_rows)
    grad_rows = grad_out.reshape(blocks, TOK_DEV, HD)
    cumulative = jnp.cumsum(log_decay.reshape(HEADS, blocks, TOK_DEV).transpose(1, 0, 2), axis=2)
    block_total = cumulative[:, :, -1]

    def local_fn(operands):
        k_heads, v_heads, cumul, last_value = operands
        tail = jnp.exp(last_value[:, None] - cumul)
        return exact_product('htd,hte->hde', k_heads.astype(jnp.float32) * tail[..., None], v_heads)
    local_state = lax.map(local_fn, (k_all, v_all, cumulative, block_total))

    def carry_step(carry, operands):
        decay_total, local_term = operands
        return (decay_total[:, None, None] * carry + local_term, carry)
    zero_state = jnp.zeros((HEADS, DH, DH), jnp.float32)
    _, state_in = lax.scan(carry_step, zero_state, (jnp.exp(block_total), local_state))

    def second_pass(operands):
        q_heads, k_heads, v_heads, grad_block, cumul, state = operands
        attended, _, _ = attend(q_heads, k_heads, v_heads, cumul, state)
        normed, grad_heads = normalize(attended, grad_block, norm_gain)
        output_block = (normed * norm_gain[None, :]).astype(jnp.bfloat16)
        gain_part = lax.optimization_barrier(jnp.sum(grad_block.astype(jnp.float32) * normed, axis=0))
        state_grad = exact_product('htd,hte->hde', q_heads.astype(jnp.float32) * jnp.exp(cumul)[..., None], grad_heads)
        return (output_block, gain_part, state_grad)
    output, gain_parts, state_grad = lax.map(second_pass, (q_all, k_all, v_all, grad_rows, cumulative, state_in))
    _, state_after = lax.scan(carry_step, zero_state, (jnp.exp(block_total), state_grad), reverse=True)

    def fourth_pass(operands):
        q_heads, k_heads, v_heads, grad_block, cumul, last_value, state, after = operands
        attended, weights, decay_mask = attend(q_heads, k_heads, v_heads, cumul, state)
        _, grad_heads = normalize(attended, grad_block, norm_gain)
        grad_weights = (plain_product('htd,hsd->hts', grad_heads, v_heads) * decay_mask).astype(jnp.bfloat16)
        tail = jnp.exp(last_value[:, None] - cumul)[..., None]
        grad_q = plain_product('hts,hsd->htd', grad_weights, k_heads)
        grad_q = grad_q + jnp.exp(cumul)[..., None] * exact_product('hte,hde->htd', grad_heads, state)
        grad_k = plain_product('hts,htd->hsd', grad_weights, q_heads)
        grad_k = grad_k + tail * exact_product('hse,hde->hsd', v_heads, after)
        grad_v = plain_product('hts,htd->hsd', weights, grad_heads)
        grad_v = grad_v + tail * exact_product('hsd,hde->hse', k_heads, after)
        return (merge_heads(grad_q).astype(jnp.bfloat16), merge_heads(grad_k).astype(jnp.bfloat16), merge_heads(grad_v).astype(jnp.bfloat16))
    grad_q, grad_k, grad_v = lax.map(fourth_pass, (q_all, k_all, v_all, grad_rows, cumulative, block_total, state_in, state_after))
    grad_gain = lax.optimization_barrier(jnp.sum(gain_parts, axis=0))
    return (output.reshape(SEQUENCE_TOKENS, HD), grad_q.reshape(SEQUENCE_TOKENS, HD), grad_k.reshape(SEQUENCE_TOKENS, HD), grad_v.reshape(SEQUENCE_TOKENS, HD), grad_gain)
```

```python
import functools

import jax
import jax.numpy as jnp
from jax import lax
from jax.experimental import pallas as pl
from jax.experimental.pallas import tpu as pltpu
from jax.sharding import Mesh
from jax.sharding import PartitionSpec as P

DH = 128
HD = 8192
EPSILON = 1e-06
CHUNK = 256
SEQ = ("seq_0", "seq_1", "seq_2")
F32 = jnp.float32
BF16 = jnp.bfloat16


def dot(a, b, ca, cb, precision=None):
    return lax.dot_general(
        a, b, (((ca,), (cb,)), ((), ())), precision=precision, preferred_element_type=F32
    )


def lane_prefix(x):
    n = x.shape[1]
    lane = lax.broadcasted_iota(jnp.int32, x.shape, 1)
    step = 1
    while step < n:
        x = x + jnp.where(lane >= step, pltpu.roll(x, step, 1), 0.0)
        step *= 2
    return x


def columns(cum_t_ref, first):
    return pltpu.roll(cum_t_ref[...], lax.rem(128 - first, 128), 1)


def head(ref, i):
    return ref[:, i * DH : (i + 1) * DH]


def local_kernel(hp, ld_ref, k_ref, v_ref, state_ref, cum_ref, cum_t_ref):
    step = pl.program_id(0)

    @pl.when(step == 0)
    def _():
        cum = lane_prefix(ld_ref[...])
        cum_ref[...] = cum
        heads = cum.shape[0]
        padded = jnp.concatenate([cum, jnp.zeros((128 - heads, cum.shape[1]), F32)], axis=0)
        cum_t_ref[...] = padded.T

    col = columns(cum_t_ref, step * hp)
    end = col[-1:, :]
    tail = jnp.exp(end - col)
    total = jnp.exp(end)
    for i in range(hp):
        k = (head(k_ref, i).astype(F32) * tail[:, i : i + 1]).astype(BF16)
        s = dot(k, head(v_ref, i), 0, 0)
        decay = jnp.broadcast_to(total[:, i : i + 1], (8, 128))
        for half in range(2):
            state_ref[2 * i + half, 0:64] = s[64 * half : 64 * half + 64]
            state_ref[2 * i + half, 64:72] = decay


def weights_of(q, k, col, row):
    t = lax.broadcasted_iota(jnp.int32, (CHUNK, CHUNK), 0)
    s = lax.broadcasted_iota(jnp.int32, (CHUNK, CHUNK), 1)
    decay = jnp.where(t >= s, jnp.exp(col - row), 0.0)
    return decay, (dot(q, k, 1, 1) * decay).astype(BF16)


def forward_kernel(hp, n, cum_ref, cum_t_ref, q_ref, k_ref, v_ref, out_ref):
    step = pl.program_id(0)
    cols = columns(cum_t_ref, step * hp)
    for i in range(hp):
        state = None
        base = jnp.zeros((1, 1), F32)
        for j in range(n):
            at = slice(j * CHUNK, (j + 1) * CHUNK)
            col = cols[at, i : i + 1]
            end = col[CHUNK - 1 :, :]
            row = cum_ref[0, i : i + 1, at]
            lanes = slice(i * DH, (i + 1) * DH)
            q, k, v = q_ref[at, lanes], k_ref[at, lanes], v_ref[at, lanes]
            _, w = weights_of(q, k, col, row)
            a = dot(w, v, 1, 0)
            if j > 0:
                a = a + jnp.exp(col - base) * dot(q, state.astype(BF16), 1, 0)
            out_ref[at, lanes] = a.astype(BF16)
            if j < n - 1:
                kd = (k.astype(F32) * jnp.exp(end - col)).astype(BF16)
                new = dot(kd, v, 0, 0)
                state = new if state is None else state * jnp.exp(end - base) + new
            base = end


def sums_kernel(hp, cum_t_ref, q_ref, g_ref, a_ref, s_ref, gain_ref, att_ref, sum_ref, sq, cross):
    step = pl.program_id(0)

    @pl.when(step == 0)
    def _():
        sq[...] = jnp.zeros_like(sq)
        cross[...] = jnp.zeros_like(cross)

    growth = jnp.exp(columns(cum_t_ref, step * hp))
    sq_sum, cross_sum = sq[...], cross[...]
    for i in range(hp):
        att = head(a_ref, i).astype(F32) + growth[:, i : i + 1] * dot(
            head(q_ref, i), s_ref[i].astype(BF16), 1, 0
        )
        att_ref[:, i * DH : (i + 1) * DH] = att.astype(BF16)
        gg = head(g_ref, i).astype(F32) * head(gain_ref, i)
        sq_sum = sq_sum + att * att
        cross_sum = cross_sum + gg * att
    sq[...] = sq_sum
    cross[...] = cross_sum

    @pl.when(step == pl.num_programs(0) - 1)
    def _():
        a = jnp.sum(sq[...].T, axis=0, keepdims=True)
        b = jnp.sum(cross[...].T, axis=0, keepdims=True)
        which = lax.broadcasted_iota(jnp.int32, sum_ref.shape, 0)
        sum_ref[...] = jnp.where(which == 0, a, b)


def grad_kernel(
    hp, cum_t_ref, q_ref, g_ref, a_ref, gain_ref, s0, s1, s2, s3, ga_ref, state_ref, inv_ref, beta
):
    step = pl.program_id(0)

    @pl.when(step == 0)
    def _():
        sums = (s0[...] + s1[...]) + (s2[...] + s3[...])
        inverse = lax.rsqrt(sums[0:1] / HD + EPSILON)
        center = sums[1:2] * inverse / HD
        both = inverse * inverse * center
        length = both.shape[1]
        inv_ref[...] = jnp.broadcast_to(inverse, (128, length)).T
        beta[...] = jnp.broadcast_to(both, (128, length)).T

    growth = jnp.exp(columns(cum_t_ref, step * hp))
    inverse, both = inv_ref[...], beta[...]
    for i in range(hp):
        att = head(a_ref, i).astype(F32)
        scaled = head(g_ref, i).astype(F32) * inverse
        ga = (scaled * head(gain_ref, i) - both * att).astype(BF16)
        ga_ref[:, i * DH : (i + 1) * DH] = ga
        gain_part = jnp.sum(scaled * att, axis=0, keepdims=True)
        qd = (head(q_ref, i).astype(F32) * growth[:, i : i + 1]).astype(BF16)
        s = dot(qd, ga, 0, 0)
        for half in range(2):
            state_ref[2 * i + half, 0:64] = s[64 * half : 64 * half + 64]
            state_ref[2 * i + half, 64:72] = jnp.broadcast_to(gain_part, (8, 128))


def backward_kernel(
    hp, n, cum_ref, cum_t_ref, inv_ref, gain_ref, q_ref, k_ref, v_ref, ga_ref, a_ref, s_ref,
    out_ref, gq_ref, gk_ref, gv_ref,
):
    step = pl.program_id(0)
    cols = columns(cum_t_ref, step * hp)
    for i in range(hp):
        lanes = slice(i * DH, (i + 1) * DH)
        out_ref[:, lanes] = (
            head(a_ref, i).astype(F32) * inv_ref[...] * head(gain_ref, i)
        ).astype(BF16)
        states = [s_ref[i]]
        ends = [jnp.zeros((1, 1), F32)]
        for j in range(n):
            at = slice(j * CHUNK, (j + 1) * CHUNK)
            col = cols[at, i : i + 1]
            end = col[CHUNK - 1 :, :]
            if j < n - 1:
                kd = (k_ref[at, lanes].astype(F32) * jnp.exp(end - col)).astype(BF16)
                states.append(
                    states[-1] * jnp.exp(end - ends[-1]) + dot(kd, v_ref[at, lanes], 0, 0)
                )
            ends.append(end)
        after = None
        for j in reversed(range(n)):
            at = slice(j * CHUNK, (j + 1) * CHUNK)
            col = cols[at, i : i + 1]
            row = cum_ref[0, i : i + 1, at]
            q, k, v, ga = q_ref[at, lanes], k_ref[at, lanes], v_ref[at, lanes], ga_ref[at, lanes]
            decay, w = weights_of(q, k, col, row)
            gw = (dot(ga, v, 1, 1) * decay).astype(BF16)
            grow = jnp.exp(col - ends[j])
            gq = dot(gw, k, 1, 0) + grow * dot(ga, states[j].astype(BF16), 1, 1)
            gk = dot(gw, q, 0, 0)
            gv = dot(w, ga, 0, 0)
            if after is not None:
                tail = jnp.exp(ends[j + 1] - col)
                low = after.astype(BF16)
                gk = gk + tail * dot(v, low, 1, 1)
                gv = gv + tail * dot(k, low, 1, 0)
            gq_ref[at, lanes] = gq.astype(BF16)
            gk_ref[at, lanes] = gk.astype(BF16)
            gv_ref[at, lanes] = gv.astype(BF16)
            if j > 0:
                qd = (q.astype(F32) * grow).astype(BF16)
                new = dot(qd, ga, 0, 0)
                after = new if after is None else after * jnp.exp(ends[j + 1] - ends[j]) + new


def final_kernel(hp, cum_t_ref, k_ref, v_ref, gk_in, gv_in, s_ref, gk_ref, gv_ref):
    step = pl.program_id(0)
    col = columns(cum_t_ref, step * hp)
    tail = jnp.exp(col[-1:, :] - col)
    for i in range(hp):
        lanes = slice(i * DH, (i + 1) * DH)
        low = s_ref[i].astype(BF16)
        t = tail[:, i : i + 1]
        gk_ref[:, lanes] = (
            gk_in[:, lanes].astype(F32) + t * dot(v_ref[:, lanes], low, 1, 1)
        ).astype(BF16)
        gv_ref[:, lanes] = (
            gv_in[:, lanes].astype(F32) + t * dot(k_ref[:, lanes], low, 1, 0)
        ).astype(BF16)


def scan_forward_kernel(x_ref, out_ref):
    n = x_ref.shape[0]
    state = jnp.zeros((64, 128), F32)
    for j in range(n):
        out_ref[j] = state
        if j < n - 1:
            state = state * x_ref[j, 64:65] + x_ref[j, 0:64]


def scan_backward_kernel(d_ref, x_ref, out_ref):
    n = x_ref.shape[0]
    state = jnp.zeros((64, 128), F32)
    gain = jnp.zeros((8, 128), F32)
    for j in reversed(range(n)):
        out_ref[j, 0:64] = state
        state = state * d_ref[j, 64:65] + x_ref[j, 0:64]
        gain = gain + x_ref[j, 64:72]
    for j in range(n):
        out_ref[j, 64:72] = gain


def whole(shape):
    return pl.BlockSpec(shape, lambda h: (0,) * len(shape))


def params(limit=None):
    return pltpu.CompilerParams(
        dimension_semantics=("arbitrary",), vmem_limit_bytes=limit
    )


def cost(flops, moved, exps=0):
    return pl.CostEstimate(flops=int(flops), bytes_accessed=int(moved), transcendentals=int(exps))


def exchange(x):
    return lax.all_to_all(x, SEQ, split_axis=0, concat_axis=0, tiled=True)


def on_device(queries, key_rows, value_rows, log_decay, norm_gain, grad_out):
    tokens, width = queries.shape
    heads = width // DH
    devices = 2 * heads
    chunks = tokens // CHUNK
    gain = norm_gain[None, :]
    rows = functools.partial(jax.ShapeDtypeStruct, (tokens, width), BF16)

    def cut(hp):
        return pl.BlockSpec((tokens, hp * DH), lambda h: (0, h))

    def gain_cut(hp):
        return pl.BlockSpec((1, hp * DH), lambda h: (0, h))

    def state_cut(hp):
        return pl.BlockSpec((hp, DH, DH), lambda h: (h, 0, 0))

    def sent_cut(hp):
        return pl.BlockSpec((2 * hp, 72, DH), lambda h: (h, 0, 0))

    sent = jax.ShapeDtypeStruct((devices, 72, DH), F32)
    cum_t_spec = whole((tokens, 128))

    hp = 4
    local, cum, cum_t = pl.pallas_call(
        functools.partial(local_kernel, hp),
        grid=(heads // hp,),
        in_specs=[whole((heads, tokens)), cut(hp), cut(hp)],
        out_specs=[sent_cut(hp), whole((heads, tokens)), cum_t_spec],
        out_shape=[
            sent,
            jax.ShapeDtypeStruct((heads, tokens), F32),
            jax.ShapeDtypeStruct((tokens, 128), F32),
        ],
        compiler_params=params(),
        name="local_state",
    )(log_decay, key_rows, value_rows)

    got = exchange(local)
    hp = 2
    cum_pairs = cum.reshape(heads // hp, hp, tokens)
    pair_spec = pl.BlockSpec((1, hp, tokens), lambda h: (h, 0, 0))
    attended_local = pl.pallas_call(
        functools.partial(forward_kernel, hp, chunks),
        grid=(heads // hp,),
        in_specs=[pair_spec, cum_t_spec, cut(hp), cut(hp), cut(hp)],
        out_specs=cut(hp),
        out_shape=rows(),
        compiler_params=params(),
        cost_estimate=cost(8e9, 13e6, 3e6),
        name="forward_intra",
    )(cum_pairs, cum_t, queries, key_rows, value_rows)

    prefix = pl.pallas_call(
        scan_forward_kernel,
        out_shape=jax.ShapeDtypeStruct((devices, 64, DH), F32),
        name="scan_forward",
    )(got)
    state_in = exchange(prefix).reshape(heads, DH, DH)

    hp = 4
    attended, sums = pl.pallas_call(
        functools.partial(sums_kernel, hp),
        grid=(heads // hp,),
        in_specs=[cum_t_spec, cut(hp), cut(hp), cut(hp), state_cut(hp), gain_cut(hp)],
        out_specs=[cut(hp), whole((8, tokens))],
        out_shape=[rows(), jax.ShapeDtypeStruct((8, tokens), F32)],
        scratch_shapes=[pltpu.VMEM((tokens, 128), F32), pltpu.VMEM((tokens, 128), F32)],
        compiler_params=params(),
        name="row_sums",
    )(cum_t, queries, grad_out, attended_local, state_in, gain)

    groups = lax.axis_size("head")
    others = [
        lax.ppermute(sums, "head", [(i, (i + shift) % groups) for i in range(groups)])
        for shift in range(1, groups)
    ]

    grad_attended, sent_grad, inverse = pl.pallas_call(
        functools.partial(grad_kernel, hp),
        grid=(heads // hp,),
        in_specs=[cum_t_spec, cut(hp), cut(hp), cut(hp), gain_cut(hp)]
        + [whole((8, tokens))] * 4,
        out_specs=[cut(hp), sent_cut(hp), cum_t_spec],
        out_shape=[rows(), sent, jax.ShapeDtypeStruct((tokens, 128), F32)],
        scratch_shapes=[pltpu.VMEM((tokens, 128), F32)],
        compiler_params=params(),
        name="grad_state",
    )(cum_t, queries, grad_out, attended, gain, sums, *others)

    got_grad = exchange(sent_grad)
    hp = 2
    output, grad_q, part_k, part_v = pl.pallas_call(
        functools.partial(backward_kernel, hp, chunks),
        grid=(heads // hp,),
        in_specs=[pair_spec, cum_t_spec, cum_t_spec, gain_cut(hp)]
        + [cut(hp)] * 5
        + [state_cut(hp)],
        out_specs=[cut(hp)] * 4,
        out_shape=[rows()] * 4,
        compiler_params=params(),
        cost_estimate=cost(20e9, 30e6, 3e6),
        name="backward_intra",
    )(
        cum_pairs, cum_t, inverse, gain, queries, key_rows, value_rows, grad_attended, attended,
        state_in,
    )

    suffix = pl.pallas_call(
        scan_backward_kernel,
        out_shape=sent,
        name="scan_backward",
    )(got, got_grad)
    back = exchange(suffix)
    state_after = back[:, 0:64].reshape(heads, DH, DH)
    grad_gain = back[0::2, 64].reshape(width)

    hp = 4
    grad_k, grad_v = pl.pallas_call(
        functools.partial(final_kernel, hp),
        grid=(heads // hp,),
        in_specs=[cum_t_spec] + [cut(hp)] * 4 + [state_cut(hp)],
        out_specs=[cut(hp)] * 2,
        out_shape=[rows()] * 2,
        input_output_aliases={3: 0, 4: 1},
        compiler_params=params(),
        name="final_grads",
    )(cum_t, key_rows, value_rows, part_k, part_v, state_after)
    return output, grad_q, grad_k, grad_v, grad_gain


def solution(mesh):
    split = Mesh(
        mesh.devices.reshape(4, 4, 2, mesh.shape["head"]), ("seq_0", "seq_1", "seq_2", "head")
    )
    placed = (
        P(SEQ, "head"),
        P(SEQ, "head"),
        P(SEQ, "head"),
        P("head", SEQ),
        P("head"),
        P(SEQ, "head"),
    )
    return jax.shard_map(
        on_device,
        mesh=split,
        in_specs=placed,
        out_specs=(P(SEQ, "head"), P(SEQ, "head"), P(SEQ, "head"), P(SEQ, "head"), P("head")),
        check_vma=False,
    )
```

```python
import functools

import jax
import jax.numpy as jnp
from jax import lax
from jax.experimental import pallas as pl
from jax.experimental.pallas import tpu as pltpu
from jax.sharding import Mesh
from jax.sharding import PartitionSpec as P

DH = 128
HD = 8192
EPSILON = 1e-06
CHUNK = 256
LIMIT = 25 * 10**6
SEQ = ("seq_0", "seq_1", "seq_2")
F32 = jnp.float32
BF16 = jnp.bfloat16


def dot(a, b, ca, cb, precision=None):
    return lax.dot_general(
        a, b, (((ca,), (cb,)), ((), ())), precision=precision, preferred_element_type=F32
    )


def lane_prefix(x):
    rows, n = x.shape
    high = x.astype(BF16)
    rest = x - high.astype(F32)
    middle = rest.astype(BF16)
    low = (rest - middle.astype(F32)).astype(BF16)
    blocks = n // 128
    parts = [p[:, 128 * b : 128 * b + 128] for b in range(blocks) for p in (high, middle, low)]
    stacked = jnp.concatenate(parts, axis=0)
    s = lax.broadcasted_iota(jnp.int32, (128, 128), 0)
    t = lax.broadcasted_iota(jnp.int32, (128, 128), 1)
    sums = dot(stacked, (s <= t).astype(BF16), 1, 0)
    out, before = [], jnp.zeros((rows, 1), F32)
    for b in range(blocks):
        first = 3 * rows * b
        inside = (
            sums[first : first + rows]
            + (sums[first + rows : first + 2 * rows] + sums[first + 2 * rows : first + 3 * rows])
        )
        out.append(inside + before)
        before = out[-1][:, 127:]
    return jnp.concatenate(out, axis=1)


def columns(cum_t_ref, first):
    return pltpu.roll(cum_t_ref[...], lax.rem(128 - first, 128), 1)


def head(ref, i):
    return ref[:, i * DH : (i + 1) * DH]


def local_kernel(hp, ld_ref, k_ref, v_ref, state_ref, cum_ref, cum_t_ref):
    step = pl.program_id(0)

    @pl.when(step == 0)
    def _():
        cum = lane_prefix(ld_ref[...])
        cum_ref[...] = cum
        heads = cum.shape[0]
        padded = jnp.concatenate([cum, jnp.zeros((128 - heads, cum.shape[1]), F32)], axis=0)
        cum_t_ref[...] = padded.T

    col = columns(cum_t_ref, step * hp)
    end = col[-1:, :]
    tail = jnp.exp(end - col)
    total = jnp.exp(end)
    for i in range(hp):
        k = (head(k_ref, i).astype(F32) * tail[:, i : i + 1]).astype(BF16)
        s = dot(k, head(v_ref, i), 0, 0)
        decay = jnp.broadcast_to(total[:, i : i + 1], (8, 128))
        for half in range(2):
            state_ref[2 * i + half, 0:64] = s[64 * half : 64 * half + 64]
            state_ref[2 * i + half, 64:72] = decay


def weights_of(q, k, col, row):
    t = lax.broadcasted_iota(jnp.int32, (CHUNK, CHUNK), 0)
    s = lax.broadcasted_iota(jnp.int32, (CHUNK, CHUNK), 1)
    decay = jnp.where(t >= s, jnp.exp(col - row), 0.0)
    return decay, (dot(q, k, 1, 1) * decay).astype(BF16)


def forward_kernel(hp, n, cum_ref, cum_t_ref, q_ref, k_ref, v_ref, out_ref):
    step = pl.program_id(0)
    cols = columns(cum_t_ref, step * hp)
    for i in range(hp):
        state = None
        base = jnp.zeros((1, 1), F32)
        for j in range(n):
            at = slice(j * CHUNK, (j + 1) * CHUNK)
            col = cols[at, i : i + 1]
            end = col[CHUNK - 1 :, :]
            row = cum_ref[0, i : i + 1, at]
            lanes = slice(i * DH, (i + 1) * DH)
            q, k, v = q_ref[at, lanes], k_ref[at, lanes], v_ref[at, lanes]
            _, w = weights_of(q, k, col, row)
            a = dot(w, v, 1, 0)
            if j > 0:
                a = a + jnp.exp(col - base) * dot(q, state.astype(BF16), 1, 0)
            out_ref[at, lanes] = a.astype(BF16)
            if j < n - 1:
                kd = (k.astype(F32) * jnp.exp(end - col)).astype(BF16)
                new = dot(kd, v, 0, 0)
                state = new if state is None else state * jnp.exp(end - base) + new
            base = end


def attended_of(q, local, growth, state):
    return local.astype(F32) + growth * dot(q, state.astype(BF16), 1, 0)


def sums_kernel(hp, cum_t_ref, q_ref, g_ref, a_ref, s_ref, gain_ref, sum_ref, sq, cross):
    step = pl.program_id(0)

    @pl.when(step == 0)
    def _():
        sq[...] = jnp.zeros_like(sq)
        cross[...] = jnp.zeros_like(cross)

    growth = jnp.exp(columns(cum_t_ref, step * hp))
    sq_sum, cross_sum = sq[...], cross[...]
    for i in range(hp):
        att = attended_of(head(q_ref, i), head(a_ref, i), growth[:, i : i + 1], s_ref[i])
        gg = head(g_ref, i).astype(F32) * head(gain_ref, i)
        sq_sum = sq_sum + att * att
        cross_sum = cross_sum + gg * att
    sq[...] = sq_sum
    cross[...] = cross_sum

    @pl.when(step == pl.num_programs(0) - 1)
    def _():
        a = jnp.sum(sq[...].T, axis=0, keepdims=True)
        b = jnp.sum(cross[...].T, axis=0, keepdims=True)
        which = lax.broadcasted_iota(jnp.int32, sum_ref.shape, 0)
        sum_ref[...] = jnp.where(which == 0, a, b)


def grad_of(g, gain, att, inverse, both):
    scaled = g.astype(F32) * inverse
    return scaled, (scaled * gain - both * att).astype(BF16)


def grad_kernel(
    hp, cum_t_ref, q_ref, g_ref, a_ref, s_ref, gain_ref, s0, s1, s2, s3, state_ref, inv_ref,
    both_ref,
):
    step = pl.program_id(0)

    @pl.when(step == 0)
    def _():
        sums = (s0[...] + s1[...]) + (s2[...] + s3[...])
        inverse = lax.rsqrt(sums[0:1] / HD + EPSILON)
        center = sums[1:2] * inverse / HD
        both = inverse * inverse * center
        length = both.shape[1]
        inv_ref[...] = jnp.broadcast_to(inverse, (128, length)).T
        both_ref[...] = jnp.broadcast_to(both, (128, length)).T

    growth = jnp.exp(columns(cum_t_ref, step * hp))
    inverse, both = inv_ref[...], both_ref[...]
    for i in range(hp):
        grow = growth[:, i : i + 1]
        att = attended_of(head(q_ref, i), head(a_ref, i), grow, s_ref[i])
        scaled, ga = grad_of(head(g_ref, i), head(gain_ref, i), att, inverse, both)
        gain_part = jnp.sum(scaled * att, axis=0, keepdims=True)
        qd = (head(q_ref, i).astype(F32) * grow).astype(BF16)
        s = dot(qd, ga, 0, 0)
        for half in range(2):
            state_ref[2 * i + half, 0:64] = s[64 * half : 64 * half + 64]
            state_ref[2 * i + half, 64:72] = jnp.broadcast_to(gain_part, (8, 128))


def backward_kernel(
    hp, n, first, cum_ref, cum_t_ref, inv_ref, both_ref, gain_ref, q_ref, k_ref, v_ref, g_ref,
    a_ref, s_ref, *refs,
):
    out_ref, gq_ref, gk_ref, gv_ref, mark_ref = refs[-5:]
    mark_ref[...] = jnp.zeros_like(mark_ref)
    step = pl.program_id(0) + first
    cols = columns(cum_t_ref, step * hp)
    for i in range(hp):
        lanes = slice(i * DH, (i + 1) * DH)
        att = attended_of(head(q_ref, i), head(a_ref, i), jnp.exp(cols[:, i : i + 1]), s_ref[i])
        inverse = inv_ref[...]
        out_ref[:, lanes] = (att * inverse * head(gain_ref, i)).astype(BF16)
        ga_all = grad_of(head(g_ref, i), head(gain_ref, i), att, inverse, both_ref[...])[1]
        states = [s_ref[i]]
        ends = [jnp.zeros((1, 1), F32)]
        for j in range(n):
            at = slice(j * CHUNK, (j + 1) * CHUNK)
            col = cols[at, i : i + 1]
            end = col[CHUNK - 1 :, :]
            if j < n - 1:
                kd = (k_ref[at, lanes].astype(F32) * jnp.exp(end - col)).astype(BF16)
                states.append(
                    states[-1] * jnp.exp(end - ends[-1]) + dot(kd, v_ref[at, lanes], 0, 0)
                )
            ends.append(end)
        after = None
        for j in reversed(range(n)):
            at = slice(j * CHUNK, (j + 1) * CHUNK)
            col = cols[at, i : i + 1]
            row = cum_ref[0, i : i + 1, at]
            q, k, v, ga = q_ref[at, lanes], k_ref[at, lanes], v_ref[at, lanes], ga_all[at]
            decay, w = weights_of(q, k, col, row)
            gw = (dot(ga, v, 1, 1) * decay).astype(BF16)
            grow = jnp.exp(col - ends[j])
            gq = dot(gw, k, 1, 0) + grow * dot(ga, states[j].astype(BF16), 1, 1)
            gk = dot(gw, q, 0, 0)
            gv = dot(w, ga, 0, 0)
            if after is not None:
                tail = jnp.exp(ends[j + 1] - col)
                low = after.astype(BF16)
                gk = gk + tail * dot(v, low, 1, 1)
                gv = gv + tail * dot(k, low, 1, 0)
            gq_ref[at, lanes] = gq.astype(BF16)
            gk_ref[at, lanes] = gk.astype(BF16)
            gv_ref[at, lanes] = gv.astype(BF16)
            if j > 0:
                qd = (q.astype(F32) * grow).astype(BF16)
                new = dot(qd, ga, 0, 0)
                after = new if after is None else after * jnp.exp(ends[j + 1] - ends[j]) + new


def final_kernel(hp, cum_t_ref, k_ref, v_ref, gk_in, gv_in, s_ref, gk_ref, gv_ref):
    step = pl.program_id(0)
    col = columns(cum_t_ref, step * hp)
    tail = jnp.exp(col[-1:, :] - col)
    for i in range(hp):
        lanes = slice(i * DH, (i + 1) * DH)
        low = jnp.concatenate([s_ref[2 * i, 0:64], s_ref[2 * i + 1, 0:64]], axis=0).astype(BF16)
        t = tail[:, i : i + 1]
        gk_ref[:, lanes] = (
            gk_in[:, lanes].astype(F32) + t * dot(v_ref[:, lanes], low, 1, 1)
        ).astype(BF16)
        gv_ref[:, lanes] = (
            gv_in[:, lanes].astype(F32) + t * dot(k_ref[:, lanes], low, 1, 0)
        ).astype(BF16)


def scan_forward_kernel(x_ref, out_ref):
    n = x_ref.shape[0]
    state = jnp.zeros((64, 128), F32)
    for j in range(n):
        out_ref[j] = state
        if j < n - 1:
            state = state * x_ref[j, 64:65] + x_ref[j, 0:64]


def scan_backward_kernel(d_ref, x_ref, mark_ref, out_ref):
    n = x_ref.shape[0]
    state = jnp.zeros((64, 128), F32)
    gain = jnp.zeros((8, 128), F32)
    for j in reversed(range(n)):
        out_ref[j, 0:64] = state
        state = state * d_ref[j, 64:65] + x_ref[j, 0:64]
        gain = gain + x_ref[j, 64:72]
    for j in range(n):
        out_ref[j, 64:72] = gain


def whole(shape):
    return pl.BlockSpec(shape, lambda h: (0,) * len(shape))


def params(limit=LIMIT):
    return pltpu.CompilerParams(
        dimension_semantics=("arbitrary",), vmem_limit_bytes=limit
    )


def cost(flops, moved, exps=0):
    return pl.CostEstimate(flops=int(flops), bytes_accessed=int(moved), transcendentals=int(exps))


def far(x):
    return pltpu.with_memory_space_constraint(x, pltpu.HBM)


def exchange(x):
    return lax.all_to_all(x, SEQ, split_axis=0, concat_axis=0, tiled=True)


def other_heads(sums):
    groups = lax.axis_size("head")
    return [
        lax.ppermute(sums, "head", [(i, (i + shift) % groups) for i in range(groups)])
        for shift in range(1, groups)
    ]


def on_device(queries, key_rows, value_rows, log_decay, norm_gain, grad_out):
    tokens, width = queries.shape
    heads = width // DH
    devices = 2 * heads
    chunks = tokens // CHUNK
    gain = norm_gain[None, :]
    rows = functools.partial(pltpu.HBM, (tokens, width), BF16)
    queries, key_rows, value_rows, grad_out = map(far, (queries, key_rows, value_rows, grad_out))

    def cut(hp):
        return pl.BlockSpec((tokens, hp * DH), lambda h: (0, h))

    def gain_cut(hp):
        return pl.BlockSpec((1, hp * DH), lambda h: (0, h))

    def state_cut(hp):
        return pl.BlockSpec((hp, DH, DH), lambda h: (h, 0, 0))

    def sent_cut(hp):
        return pl.BlockSpec((2 * hp, 72, DH), lambda h: (h, 0, 0))

    sent = pltpu.HBM((devices, 72, DH), F32)
    cum_t_spec = whole((tokens, 128))

    hp = 4
    local, cum, cum_t = pl.pallas_call(
        functools.partial(local_kernel, hp),
        grid=(heads // hp,),
        in_specs=[whole((heads, tokens)), cut(hp), cut(hp)],
        out_specs=[sent_cut(hp), whole((heads, tokens)), cum_t_spec],
        out_shape=[
            sent,
            pltpu.HBM((heads, tokens), F32),
            pltpu.HBM((tokens, 128), F32),
        ],
        compiler_params=params(),
        name="local_state",
    )(log_decay, key_rows, value_rows)

    got = exchange(local)
    hp = 2
    cum_pairs = cum.reshape(heads // hp, hp, tokens)
    pair_spec = pl.BlockSpec((1, hp, tokens), lambda h: (h, 0, 0))
    attended_local = pl.pallas_call(
        functools.partial(forward_kernel, hp, chunks),
        grid=(heads // hp,),
        in_specs=[pair_spec, cum_t_spec, cut(hp), cut(hp), cut(hp)],
        out_specs=cut(hp),
        out_shape=rows(),
        compiler_params=params(),
        cost_estimate=cost(8e9, 13e6, 3e6),
        name="forward_intra",
    )(cum_pairs, far(cum_t), queries, key_rows, value_rows)

    prefix = pl.pallas_call(
        scan_forward_kernel,
        out_shape=pltpu.HBM((devices, 64, DH), F32),
        compiler_params=pltpu.CompilerParams(vmem_limit_bytes=LIMIT),
        name="scan_forward",
    )(got)
    state_in = exchange(prefix).reshape(heads, DH, DH)

    hp = 4
    sums = pl.pallas_call(
        functools.partial(sums_kernel, hp),
        grid=(heads // hp,),
        in_specs=[cum_t_spec, cut(hp), cut(hp), cut(hp), state_cut(hp), gain_cut(hp)],
        out_specs=whole((8, tokens)),
        out_shape=jax.ShapeDtypeStruct((8, tokens), F32),
        scratch_shapes=[pltpu.VMEM((tokens, 128), F32), pltpu.VMEM((tokens, 128), F32)],
        compiler_params=params(),
        name="row_sums",
    )(far(cum_t), queries, grad_out, far(attended_local), state_in, gain)

    others = other_heads(sums)
    column = pltpu.HBM((tokens, 128), F32)
    sent_grad, inverse, both = pl.pallas_call(
        functools.partial(grad_kernel, hp),
        grid=(heads // hp,),
        in_specs=[cum_t_spec, cut(hp), cut(hp), cut(hp), state_cut(hp), gain_cut(hp)]
        + [whole((8, tokens))] * 4,
        out_specs=[sent_cut(hp), cum_t_spec, cum_t_spec],
        out_shape=[sent, column, column],
        compiler_params=params(),
        name="grad_state",
    )(far(cum_t), queries, grad_out, far(attended_local), state_in, gain, sums, *others)

    got_grad = exchange(sent_grad)
    hp = 2
    halves = 2
    steps = heads // hp // halves
    done = []
    for part in range(halves):
        first = part * steps

        def block(hp, first=first):
            return pl.BlockSpec((tokens, hp * DH), lambda h: (0, h + first))

        *done, mark = pl.pallas_call(
            functools.partial(backward_kernel, hp, chunks, first),
            grid=(steps,),
            in_specs=[
                pl.BlockSpec((1, hp, tokens), lambda h, first=first: (h + first, 0, 0)),
                cum_t_spec,
                cum_t_spec,
                cum_t_spec,
                pl.BlockSpec((1, hp * DH), lambda h, first=first: (0, h + first)),
            ]
            + [block(hp)] * 5
            + [pl.BlockSpec((hp, DH, DH), lambda h, first=first: (h + first, 0, 0))]
            + [pl.BlockSpec(memory_space=pl.ANY)] * len(done),
            out_specs=[block(hp)] * 4 + [whole((8, 128))],
            out_shape=[rows()] * 4 + [jax.ShapeDtypeStruct((8, 128), F32)],
            input_output_aliases={11 + i: i for i in range(len(done))},
            compiler_params=params(),
            cost_estimate=cost(10e9, 15e6, 2e6),
            name="backward_intra",
        )(
            cum_pairs, far(cum_t), far(inverse), far(both), gain, queries, key_rows, value_rows,
            grad_out, far(attended_local), state_in, *map(far, done),
        )
        if part == 0:
            first_mark = mark
    output, grad_q, part_k, part_v = done

    suffix = pl.pallas_call(
        scan_backward_kernel,
        out_shape=sent,
        compiler_params=pltpu.CompilerParams(vmem_limit_bytes=LIMIT),
        name="scan_backward",
    )(far(got), got_grad, first_mark)
    back = exchange(suffix)
    grad_gain = back[0::2, 64].reshape(width)

    hp = 4
    grad_k, grad_v = pl.pallas_call(
        functools.partial(final_kernel, hp),
        grid=(heads // hp,),
        in_specs=[cum_t_spec] + [cut(hp)] * 4 + [sent_cut(hp)],
        out_specs=[cut(hp)] * 2,
        out_shape=[rows()] * 2,
        input_output_aliases={3: 0, 4: 1},
        compiler_params=params(),
        name="final_grads",
    )(far(cum_t), key_rows, value_rows, far(part_k), far(part_v), back)
    return output, grad_q, grad_k, grad_v, grad_gain


def solution(mesh):
    split = Mesh(
        mesh.devices.reshape(4, 4, 2, mesh.shape["head"]), ("seq_0", "seq_1", "seq_2", "head")
    )
    placed = (
        P(SEQ, "head"),
        P(SEQ, "head"),
        P(SEQ, "head"),
        P("head", SEQ),
        P("head"),
        P(SEQ, "head"),
    )
    return jax.shard_map(
        on_device,
        mesh=split,
        in_specs=placed,
        out_specs=(P(SEQ, "head"), P(SEQ, "head"), P(SEQ, "head"), P(SEQ, "head"), P("head")),
        check_vma=False,
    )
```

```python
import functools

import jax
import jax.numpy as jnp
from jax import lax
from jax.experimental import pallas as pl
from jax.experimental.pallas import tpu as pltpu
from jax.sharding import Mesh
from jax.sharding import PartitionSpec as P

DH = 128
HD = 8192
EPSILON = 1e-06
CHUNK = 256
LIMIT = 26 * 10**6
SEQ = ("seq_0", "seq_1", "seq_2")
F32 = jnp.float32
BF16 = jnp.bfloat16


def dot(a, b, ca, cb, precision=None):
    return lax.dot_general(
        a, b, (((ca,), (cb,)), ((), ())), precision=precision, preferred_element_type=F32
    )


def lane_prefix(x):
    rows, n = x.shape
    high = x.astype(BF16)
    rest = x - high.astype(F32)
    middle = rest.astype(BF16)
    low = (rest - middle.astype(F32)).astype(BF16)
    blocks = n // 128
    parts = [p[:, 128 * b : 128 * b + 128] for b in range(blocks) for p in (high, middle, low)]
    stacked = jnp.concatenate(parts, axis=0)
    s = lax.broadcasted_iota(jnp.int32, (128, 128), 0)
    t = lax.broadcasted_iota(jnp.int32, (128, 128), 1)
    sums = dot(stacked, (s <= t).astype(BF16), 1, 0)
    out, before = [], jnp.zeros((rows, 1), F32)
    for b in range(blocks):
        first = 3 * rows * b
        inside = (
            sums[first : first + rows]
            + (sums[first + rows : first + 2 * rows] + sums[first + 2 * rows : first + 3 * rows])
        )
        out.append(inside + before)
        before = out[-1][:, 127:]
    return jnp.concatenate(out, axis=1)


def turn(rows_of):
    heads, n = rows_of.shape
    return jnp.concatenate([rows_of, jnp.zeros((128 - heads, n), F32)], axis=0).T


def columns(cum_t_ref, first):
    return pltpu.roll(cum_t_ref[...], lax.rem(128 - first, 128), 1)


def pair(first, second):
    zero = jnp.zeros_like(first)
    return jnp.concatenate(
        [jnp.concatenate([first, zero], axis=1), jnp.concatenate([zero, second], axis=1)], axis=0
    )


def lanes_of(h, n=1):
    return pl.ds(pl.multiple_of(h * DH, DH), n * DH)


def over_heads(count, step, body):
    lax.fori_loop(0, count // step, lambda i, c: (body(i, i * step), c)[1], 0)


def copy_piece(source, target, sems, i, n):
    at = lanes_of(i * n, n)
    return pltpu.make_async_copy(source.at[:, at], target.at[:, at], sems.at[i])


def send_state(state_ref, h, s, extra):
    for half in range(2):
        state_ref[2 * h + half, 0:64] = s[64 * half : 64 * half + 64]
        state_ref[2 * h + half, 64:72] = jnp.broadcast_to(extra, (8, 128))


def local_kernel(hp, ld_ref, k_in, v_in, state_ref, cum_ref, k_ref, v_ref, k_sem, v_sem):
    heads = ld_ref.shape[0]
    for i in range(heads // hp):
        copy_piece(k_in, k_ref, k_sem, i, hp).start()
        copy_piece(v_in, v_ref, v_sem, i, hp).start()
    cum_ref[...] = lane_prefix(ld_ref[...])

    def body(i, first):
        copy_piece(k_in, k_ref, k_sem, i, hp).wait()
        copy_piece(v_in, v_ref, v_sem, i, hp).wait()
        for j in range(hp):
            at = lanes_of(first + j)
            row = cum_ref[pl.ds(first + j, 1), :]
            end = row[:, -1:]
            k = (k_ref[:, at].T.astype(F32) * jnp.exp(end - row)).astype(BF16)
            send_state(state_ref, first + j, dot(k, v_ref[:, at], 1, 0), jnp.exp(end))

    over_heads(heads, hp, body)


def weights_of(q, k, col, row):
    t = lax.broadcasted_iota(jnp.int32, (CHUNK, CHUNK), 0)
    s = lax.broadcasted_iota(jnp.int32, (CHUNK, CHUNK), 1)
    decay = jnp.where(t >= s, jnp.exp(col - row), 0.0)
    return decay, (dot(q, k, 1, 1) * decay).astype(BF16)


def forward_kernel(hp, n, start, cum_ref, q_in, k_in, v_in, *refs):
    out_hbm, turned_hbm, qd_hbm, kd_hbm, vd_hbm, mark_ref = refs[-17:-11]
    q_ref, k_ref, v_ref, out_ref, turned_ref, qd_ref, kd_ref, vd_ref, cum_t_ref = refs[-11:-2]
    in_sem, out_sem = refs[-2:]
    mark_ref[...] = jnp.zeros_like(mark_ref)
    count = out_ref.shape[1] // DH
    into = ((q_in, q_ref), (k_in, k_ref), (v_in, v_ref))
    out = ((out_ref, out_hbm), (qd_ref, qd_hbm), (kd_ref, kd_hbm), (vd_ref, vd_hbm))

    def spots(step):
        return lanes_of(step * hp, hp), lanes_of(start + step * hp, hp)

    def arrive(step):
        near_at, far_at = spots(step)
        return [
            pltpu.make_async_copy(a.at[:, far_at], b.at[:, near_at], in_sem.at[j, step])
            for j, (a, b) in enumerate(into)
        ]

    def leave(step):
        near_at, far_at = spots(step)
        return [
            pltpu.make_async_copy(a.at[:, near_at], b.at[:, far_at], out_sem.at[j, step])
            for j, (a, b) in enumerate(out)
        ] + [
            pltpu.make_async_copy(
                turned_ref.at[near_at], turned_hbm.at[far_at], out_sem.at[len(out), step]
            )
        ]

    for i in range(count // hp):
        for copy in arrive(i):
            copy.start()
    cum_t_ref[...] = turn(cum_ref[...])

    def body(step, first):
        for copy in arrive(step):
            copy.wait()
        cols = columns(cum_t_ref, start + first)
        growth = jnp.exp(cols)
        tail = jnp.exp(cols[-1:, :] - cols)
        for i in range(hp):
            lanes = lanes_of(first + i)
            qd = (q_ref[:, lanes].astype(F32) * growth[:, i : i + 1]).astype(BF16)
            qd_ref[:, lanes] = qd
            turned_ref[lanes, :] = qd.T
            tail_i = jnp.broadcast_to(tail[:, i : i + 1], (tail.shape[0], DH))
            kd_ref[:, lanes] = (k_ref[:, lanes].astype(F32) * tail_i).astype(BF16)
            vd_ref[:, lanes] = (v_ref[:, lanes].astype(F32) * tail_i).astype(BF16)
            state = None
            base = jnp.zeros((1, 1), F32)
            for j in range(n):
                at = slice(j * CHUNK, (j + 1) * CHUNK)
                col = cols[at, i : i + 1]
                end = col[CHUNK - 1 :, :]
                row = cum_ref[pl.ds(start + first + i, 1), at]
                q, k, v = q_ref[at, lanes], k_ref[at, lanes], v_ref[at, lanes]
                _, w = weights_of(q, k, col, row)
                a = dot(w, v, 1, 0)
                if j > 0:
                    a = a + jnp.exp(col - base) * dot(q, state.astype(BF16), 1, 0)
                out_ref[at, lanes] = a.astype(BF16)
                if j < n - 1:
                    kd = (k.astype(F32) * jnp.exp(end - col)).astype(BF16)
                    new = dot(kd, v, 0, 0)
                    state = new if state is None else state * jnp.exp(end - base) + new
                base = end
        for copy in leave(step):
            copy.start()

    over_heads(count, hp, body)
    for step in range(count // hp):
        for copy in leave(step):
            copy.wait()


def sums_kernel(
    hp, s_ref, gain_ref, q_in, g_in, a_in, turned_in, att_ref, g_ref, turned_ref, sum_ref, q_ref,
    a_ref, sq, cross, in_sem, turned_sem,
):
    heads = s_ref.shape[0]
    pairs = ((q_in, q_ref), (a_in, a_ref), (g_in, g_ref))

    def arrive(step):
        return [copy_piece(a, b, in_sem.at[j], step, hp) for j, (a, b) in enumerate(pairs)]

    for i in range(heads // hp):
        for copy in arrive(i):
            copy.start()
    turned = pltpu.make_async_copy(turned_in, turned_ref, turned_sem)
    turned.start()
    sq[...] = jnp.zeros_like(sq)
    cross[...] = jnp.zeros_like(cross)

    def body(step, first):
        for copy in arrive(step):
            copy.wait()
        sq_sum, cross_sum = sq[...], cross[...]
        for i in range(0, hp, 2):
            h = first + i
            lanes = lanes_of(h, 2)
            both = pair(s_ref[h].astype(BF16), s_ref[h + 1].astype(BF16))
            att = a_ref[:, lanes].astype(F32) + dot(q_ref[:, lanes], both, 1, 0)
            att_ref[:, lanes] = att
            gg = g_ref[:, lanes].astype(F32) * gain_ref[:, lanes]
            square, product = att * att, gg * att
            sq_sum = sq_sum + (square[:, :DH] + square[:, DH:])
            cross_sum = cross_sum + (product[:, :DH] + product[:, DH:])
        sq[...] = sq_sum
        cross[...] = cross_sum

    over_heads(heads, hp, body)
    a = jnp.sum(sq[...].T, axis=0, keepdims=True)
    b = jnp.sum(cross[...].T, axis=0, keepdims=True)
    which = lax.broadcasted_iota(jnp.int32, sum_ref.shape, 0)
    sum_ref[...] = jnp.where(which == 0, a, b)
    turned.wait()


def grad_kernel(
    hp, turned_ref, g_ref, att_ref, gain_ref, s0, s1, s2, s3, state_ref, out_hbm, ga_hbm,
    inv_ref, both_ref, out_ref, ga_ref, out_sem,
):
    sums = (s0[...] + s1[...]) + (s2[...] + s3[...])
    inverse = lax.rsqrt(sums[0:1] / HD + EPSILON)
    center = sums[1:2] * inverse / HD
    both = inverse * inverse * center
    length = both.shape[1]
    inv_ref[...] = jnp.broadcast_to(inverse, (128, length)).T
    both_ref[...] = jnp.broadcast_to(both, (128, length)).T
    heads = state_ref.shape[0] // 2

    def leave(step):
        return (
            copy_piece(out_ref, out_hbm, out_sem.at[0], step, hp),
            copy_piece(ga_ref, ga_hbm, out_sem.at[1], step, hp),
        )

    def body(step, first):
        inverse, both = inv_ref[...], both_ref[...]
        for i in range(hp):
            lanes = lanes_of(first + i)
            att = att_ref[:, lanes]
            gain = gain_ref[:, lanes]
            scaled = g_ref[:, lanes].astype(F32) * inverse
            ga = (scaled * gain - both * att).astype(BF16)
            ga_ref[:, lanes] = ga
            out_ref[:, lanes] = (att * inverse * gain).astype(BF16)
            gain_part = jnp.sum(scaled * att, axis=0, keepdims=True)
            turned = turned_ref[pl.ds(pl.multiple_of((first + i) * DH, DH), DH), :]
            send_state(state_ref, first + i, dot(turned, ga, 1, 0), gain_part)
        for copy in leave(step):
            copy.start()

    over_heads(heads, hp, body)
    for step in range(heads // hp):
        for copy in leave(step):
            copy.wait()


def backward_kernel(
    hp, n, start, cum_ref, s_ref, q_in, k_in, v_in, ga_in, *refs
):
    gq_hbm, gk_hbm, gv_hbm, mark_ref = refs[-14:-10]
    q_ref, k_ref, v_ref, ga_ref, gq_ref, gk_ref, gv_ref, cum_t_ref, in_sem, out_sem = refs[-10:]
    mark_ref[...] = jnp.zeros_like(mark_ref)
    count = gk_ref.shape[1] // DH
    into = ((q_in, q_ref), (k_in, k_ref), (v_in, v_ref), (ga_in, ga_ref))
    out = ((gq_ref, gq_hbm), (gk_ref, gk_hbm), (gv_ref, gv_hbm))

    def spots(step):
        return lanes_of(step * hp, hp), lanes_of(start + step * hp, hp)

    def arrive(step):
        near_at, far_at = spots(step)
        return [
            pltpu.make_async_copy(a.at[:, far_at], b.at[:, near_at], in_sem.at[j, step])
            for j, (a, b) in enumerate(into)
        ]

    def leave(step):
        near_at, far_at = spots(step)
        return [
            pltpu.make_async_copy(a.at[:, near_at], b.at[:, far_at], out_sem.at[j, step])
            for j, (a, b) in enumerate(out)
        ]

    for i in range(count // hp):
        for copy in arrive(i):
            copy.start()
    cum_t_ref[...] = turn(cum_ref[...])

    def body(step, first):
        for copy in arrive(step):
            copy.wait()
        cols = columns(cum_t_ref, start + first)
        for i in range(hp):
            h = start + first + i
            lanes = lanes_of(first + i)
            states = [s_ref[h]]
            ends = [jnp.zeros((1, 1), F32)]
            for j in range(n):
                at = slice(j * CHUNK, (j + 1) * CHUNK)
                col = cols[at, i : i + 1]
                end = col[CHUNK - 1 :, :]
                if j < n - 1:
                    kd = (k_ref[at, lanes].astype(F32) * jnp.exp(end - col)).astype(BF16)
                    states.append(
                        states[-1] * jnp.exp(end - ends[-1]) + dot(kd, v_ref[at, lanes], 0, 0)
                    )
                ends.append(end)
            after = None
            for j in reversed(range(n)):
                at = slice(j * CHUNK, (j + 1) * CHUNK)
                col = cols[at, i : i + 1]
                row = cum_ref[pl.ds(h, 1), at]
                q, k, v = q_ref[at, lanes], k_ref[at, lanes], v_ref[at, lanes]
                ga = ga_ref[at, lanes]
                decay, w = weights_of(q, k, col, row)
                gw = (dot(ga, v, 1, 1) * decay).astype(BF16)
                grow = jnp.exp(col - ends[j])
                gq = dot(gw, k, 1, 0) + grow * dot(ga, states[j].astype(BF16), 1, 1)
                gk = dot(gw, q, 0, 0)
                gv = dot(w, ga, 0, 0)
                if after is not None:
                    tail = jnp.exp(ends[j + 1] - col)
                    low = after.astype(BF16)
                    gk = gk + tail * dot(v, low, 1, 1)
                    gv = gv + tail * dot(k, low, 1, 0)
                gq_ref[at, lanes] = gq.astype(BF16)
                gk_ref[at, lanes] = gk.astype(BF16)
                gv_ref[at, lanes] = gv.astype(BF16)
                if j > 0:
                    qd = (q.astype(F32) * grow).astype(BF16)
                    new = dot(qd, ga, 0, 0)
                    after = new if after is None else after * jnp.exp(ends[j + 1] - ends[j]) + new
        for copy in leave(step):
            copy.start()

    over_heads(count, hp, body)
    for step in range(count // hp):
        for copy in leave(step):
            copy.wait()


def final_kernel(
    hp, s_ref, k_in, v_in, gk_in, gv_in, gk_hbm, gv_hbm,
    k_ref, v_ref, gk_ref, gv_ref, in_sem, out_sem,
):
    into = ((k_in, k_ref), (v_in, v_ref), (gk_in, gk_ref), (gv_in, gv_ref))
    heads = s_ref.shape[0] // 2

    def arrive(step):
        return [copy_piece(a, b, in_sem.at[j], step, hp) for j, (a, b) in enumerate(into)]

    def leave(step):
        return (
            copy_piece(gk_ref, gk_hbm, out_sem.at[0], step, hp),
            copy_piece(gv_ref, gv_hbm, out_sem.at[1], step, hp),
        )

    for i in range(heads // hp):
        for copy in arrive(i):
            copy.start()

    def body(step, first):
        for copy in arrive(step):
            copy.wait()
        for i in range(0, hp, 2):
            h = first + i
            lanes = lanes_of(h, 2)
            states = [
                jnp.concatenate([s_ref[2 * j, 0:64], s_ref[2 * j + 1, 0:64]], axis=0).astype(BF16)
                for j in (h, h + 1)
            ]
            both = pair(*states)
            gk_ref[:, lanes] = (
                gk_ref[:, lanes].astype(F32) + dot(v_ref[:, lanes], both, 1, 1)
            ).astype(BF16)
            gv_ref[:, lanes] = (
                gv_ref[:, lanes].astype(F32) + dot(k_ref[:, lanes], both, 1, 0)
            ).astype(BF16)
        for copy in leave(step):
            copy.start()

    over_heads(heads, hp, body)
    for step in range(heads // hp):
        for copy in leave(step):
            copy.wait()


def scan_forward_kernel(x_ref, mark_ref, out_ref):
    n = x_ref.shape[0]
    state = jnp.zeros((64, 128), F32)
    for j in range(n):
        out_ref[j] = state
        if j < n - 1:
            state = state * x_ref[j, 64:65] + x_ref[j, 0:64]


def scan_backward_kernel(d_ref, x_ref, mark_ref, out_ref):
    n = x_ref.shape[0]
    state = jnp.zeros((64, 128), F32)
    gain = jnp.zeros((8, 128), F32)
    for j in reversed(range(n)):
        out_ref[j, 0:64] = state
        state = state * d_ref[j, 64:65] + x_ref[j, 0:64]
        gain = gain + x_ref[j, 64:72]
    for j in range(n):
        out_ref[j, 64:72] = gain


def cost(flops, moved, exps=0):
    return pl.CostEstimate(flops=int(flops), bytes_accessed=int(moved), transcendentals=int(exps))


def far(x):
    return pltpu.with_memory_space_constraint(x, pltpu.HBM)


def near(x):
    return pltpu.with_memory_space_constraint(x, pltpu.VMEM)


def exchange(x):
    return lax.all_to_all(x, SEQ, split_axis=0, concat_axis=0, tiled=True)


def other_heads(sums):
    groups = lax.axis_size("head")
    return [
        lax.ppermute(sums, "head", [(i, (i + shift) % groups) for i in range(groups)])
        for shift in range(1, groups)
    ]


def on_device(queries, key_rows, value_rows, log_decay, norm_gain, grad_out):
    tokens, width = queries.shape
    heads = width // DH
    devices = 2 * heads
    chunks = tokens // CHUNK
    gain = norm_gain[None, :]
    rows = (tokens, width)
    flat = pltpu.HBM(rows, BF16)
    kept = pltpu.VMEM(rows, BF16)
    sent = pltpu.HBM((devices, 72, DH), F32)
    here = pl.BlockSpec(memory_space=pltpu.VMEM)
    there = pl.BlockSpec(memory_space=pl.ANY)
    settings = pltpu.CompilerParams(vmem_limit_bytes=LIMIT)
    queries, key_rows, value_rows, grad_out = map(far, (queries, key_rows, value_rows, grad_out))

    def sems(*n):
        return pltpu.SemaphoreType.DMA(n)

    hp = 2
    local, cum = pl.pallas_call(
        functools.partial(local_kernel, hp),
        in_specs=[here, there, there],
        out_specs=[here] * 2,
        out_shape=[sent, pltpu.HBM((heads, tokens), F32)],
        scratch_shapes=[kept] * 2 + [sems(heads // hp)] * 2,
        compiler_params=settings,
        name="local_state",
    )(far(log_decay), key_rows, value_rows)
    cum = far(cum)

    got = exchange(local)
    hp = 2
    half = heads // 2
    mark_shape = pltpu.HBM((8, 128), F32)
    cum_t_shape = pltpu.VMEM((tokens, 128), F32)
    part = pltpu.VMEM((tokens, half * DH), BF16)
    part_t = pltpu.VMEM((half * DH, tokens), BF16)
    ready, marks = [], []
    for start in (0, half):
        *ready, mark = pl.pallas_call(
            functools.partial(forward_kernel, hp, chunks, start),
            in_specs=[here] + [there] * (3 + len(ready)),
            out_specs=[there] * 5 + [here],
            out_shape=[flat, pltpu.HBM((width, tokens), BF16), flat, flat, flat, mark_shape],
            scratch_shapes=[part] * 4
            + [part_t]
            + [part] * 3
            + [cum_t_shape, sems(3, half // hp), sems(5, half // hp)],
            input_output_aliases={4 + i: i for i in range(len(ready))},
            compiler_params=settings,
            cost_estimate=cost(8e9, 13e6, 3e6),
            name="forward_intra",
        )(cum, queries, key_rows, value_rows, *map(far, ready))
        marks.append(far(mark))
    attended_local, turned, grown, faded_k, faded_v = map(far, ready)

    prefix = pl.pallas_call(
        scan_forward_kernel,
        out_shape=pltpu.HBM((devices, 64, DH), F32),
        compiler_params=settings,
        name="scan_forward",
    )(got, marks[0])
    state_in = exchange(prefix).reshape(heads, DH, DH)

    hp = 2
    attended, grads, turned, sums = pl.pallas_call(
        functools.partial(sums_kernel, hp),
        in_specs=[here] * 2 + [there] * 4,
        out_specs=[here] * 4,
        out_shape=[
            pltpu.VMEM(rows, F32),
            kept,
            pltpu.VMEM((width, tokens), BF16),
            pltpu.VMEM((8, tokens), F32),
        ],
        scratch_shapes=[kept] * 2
        + [pltpu.VMEM((tokens, 128), F32)] * 2
        + [sems(3, heads // hp), pltpu.SemaphoreType.DMA],
        compiler_params=settings,
        name="row_sums",
    )(near(state_in), gain, grown, grad_out, attended_local, turned)

    hp = 2
    others = other_heads(sums)
    sent_grad, output, grad_attended = pl.pallas_call(
        functools.partial(grad_kernel, hp),
        in_specs=[here] * 8,
        out_specs=[here] + [there] * 2,
        out_shape=[sent, flat, flat],
        scratch_shapes=[pltpu.VMEM((tokens, 128), F32)] * 2 + [kept] * 2 + [sems(2, heads // hp)],
        compiler_params=settings,
        name="grad_state",
    )(near(turned), near(grads), near(attended), gain, *map(near, (sums, *others)))

    got_grad = exchange(sent_grad)
    hp = 2
    done, marks = [], []
    for start in (0, half):
        *done, mark = pl.pallas_call(
            functools.partial(backward_kernel, hp, chunks, start),
            in_specs=[here] * 2 + [there] * (4 + len(done)),
            out_specs=[there] * 3 + [here],
            out_shape=[flat] * 3 + [mark_shape],
            scratch_shapes=[part] * 7 + [cum_t_shape, sems(4, half // hp), sems(3, half // hp)],
            input_output_aliases={6 + i: i for i in range(len(done))},
            compiler_params=settings,
            cost_estimate=cost(10e9, 15e6, 2e6),
            name="backward_intra",
        )(
            cum, far(state_in), queries, key_rows, value_rows, far(grad_attended),
            *map(far, done),
        )
        marks.append(mark)
    grad_q, part_k, part_v = done

    suffix = pl.pallas_call(
        scan_backward_kernel,
        out_shape=sent,
        compiler_params=settings,
        name="scan_backward",
    )(far(got), got_grad, far(marks[0]))
    back = exchange(suffix)
    grad_gain = back[0::2, 64].reshape(width)

    hp = 2
    grad_k, grad_v = pl.pallas_call(
        functools.partial(final_kernel, hp),
        in_specs=[here] + [there] * 4,
        out_specs=[there] * 2,
        out_shape=[flat] * 2,
        scratch_shapes=[kept] * 4 + [sems(4, heads // hp), sems(2, heads // hp)],
        compiler_params=settings,
        name="final_grads",
    )(near(back), faded_k, faded_v, far(part_k), far(part_v))
    return output, grad_q, grad_k, grad_v, grad_gain


def solution(mesh):
    split = Mesh(
        mesh.devices.reshape(4, 4, 2, mesh.shape["head"]), ("seq_0", "seq_1", "seq_2", "head")
    )
    placed = (
        P(SEQ, "head"),
        P(SEQ, "head"),
        P(SEQ, "head"),
        P("head", SEQ),
        P("head"),
        P(SEQ, "head"),
    )
    return jax.shard_map(
        on_device,
        mesh=split,
        in_specs=placed,
        out_specs=(P(SEQ, "head"), P(SEQ, "head"), P(SEQ, "head"), P(SEQ, "head"), P("head")),
        check_vma=False,
    )
```

```python
import functools

import jax
import jax.numpy as jnp
from jax import lax
from jax.experimental import pallas as pl
from jax.experimental.pallas import tpu as pltpu
from jax.sharding import Mesh
from jax.sharding import PartitionSpec as P

DH = 128
HD = 8192
EPSILON = 1e-06
CHUNK = 256
HALF = CHUNK // 2
LIMIT = 28 * 10**6
FORWARD_CUTS = (8, 8)
BACKWARD_CUTS = (8, 8)
SEQ = ("seq_0", "seq_1", "seq_2")
F32 = jnp.float32
BF16 = jnp.bfloat16


def dot(a, b, ca, cb, precision=None):
    return lax.dot_general(
        a, b, (((ca,), (cb,)), ((), ())), precision=precision, preferred_element_type=F32
    )


def lane_prefix(x):
    rows, n = x.shape
    high = x.astype(BF16)
    rest = x - high.astype(F32)
    middle = rest.astype(BF16)
    low = (rest - middle.astype(F32)).astype(BF16)
    blocks = n // 128
    parts = [p[:, 128 * b : 128 * b + 128] for b in range(blocks) for p in (high, middle, low)]
    stacked = jnp.concatenate(parts, axis=0)
    s = lax.broadcasted_iota(jnp.int32, (128, 128), 0)
    t = lax.broadcasted_iota(jnp.int32, (128, 128), 1)
    sums = dot(stacked, (s <= t).astype(BF16), 1, 0)
    out, before = [], jnp.zeros((rows, 1), F32)
    for b in range(blocks):
        first = 3 * rows * b
        inside = (
            sums[first : first + rows]
            + (sums[first + rows : first + 2 * rows] + sums[first + 2 * rows : first + 3 * rows])
        )
        out.append(inside + before)
        before = out[-1][:, 127:]
    return jnp.concatenate(out, axis=1)


def turn(rows_of):
    heads, n = rows_of.shape
    return jnp.concatenate([rows_of, jnp.zeros((128 - heads, n), F32)], axis=0).T


def columns(cum_t_ref, first):
    return pltpu.roll(cum_t_ref[...], lax.rem(128 - first, 128), 1)


def pair(first, second):
    zero = jnp.zeros_like(first)
    return jnp.concatenate(
        [jnp.concatenate([first, zero], axis=1), jnp.concatenate([zero, second], axis=1)], axis=0
    )


def lanes_of(h, n=1):
    return pl.ds(pl.multiple_of(h * DH, DH), n * DH)


def over_heads(count, step, body):
    lax.fori_loop(0, count // step, lambda i, c: (body(i, i * step), c)[1], 0)


AHEAD = 2


def begin(arrive, steps):
    for i in range(min(AHEAD, steps)):
        for copy in arrive(i):
            copy.start()


def next_piece(arrive, step, steps):
    for copy in arrive(step):
        copy.wait()

    @pl.when(step + AHEAD < steps)
    def _():
        for copy in arrive(step + AHEAD):
            copy.start()


def copy_piece(source, target, sems, i, n):
    at = lanes_of(i * n, n)
    return pltpu.make_async_copy(source.at[:, at], target.at[:, at], sems.at[i])


def send_state(state_ref, h, s, extra):
    for half in range(2):
        state_ref[2 * h + half, 0:64] = s[64 * half : 64 * half + 64]
        state_ref[2 * h + half, 64:72] = jnp.broadcast_to(extra, (8, 128))


def local_kernel(hp, ld_ref, k_in, v_in, state_ref, cum_ref, k_ref, v_ref, k_sem, v_sem):
    heads = ld_ref.shape[0]

    def arrive(i):
        return copy_piece(k_in, k_ref, k_sem, i, hp), copy_piece(v_in, v_ref, v_sem, i, hp)

    begin(arrive, heads // hp)
    cum_ref[...] = lane_prefix(ld_ref[...])

    def body(i, first):
        next_piece(arrive, i, heads // hp)
        for j in range(hp):
            at = lanes_of(first + j)
            row = cum_ref[pl.ds(first + j, 1), :]
            end = row[:, -1:]
            k = late(k_ref[:, at], row, end)
            send_state(state_ref, first + j, dot(k, v_ref[:, at], 1, 0), jnp.exp(end))

    over_heads(heads, hp, body)


def late(k, row, end):
    return (k.T.astype(F32) * jnp.exp(end - row)).astype(BF16)


def triangle(row, col):
    s = lax.broadcasted_iota(jnp.int32, (HALF, HALF), 0)
    t = lax.broadcasted_iota(jnp.int32, (HALF, HALF), 1)
    return jnp.where(s <= t, jnp.exp(row - col), 0.0)


def attend(q, k, v, col, row):
    t = lax.broadcasted_iota(jnp.int32, (CHUNK, CHUNK), 0)
    s = lax.broadcasted_iota(jnp.int32, (CHUNK, CHUNK), 1)
    decay = jnp.where(t >= s, jnp.exp(col - row), 0.0)
    return dot((dot(q, k, 1, 1) * decay).astype(BF16), v, 1, 0)


def attend_back(q, k, v, ga, col, row):
    decay = jnp.concatenate(
        [triangle(row[:, :HALF], col[:HALF]), jnp.exp(row[:, HALF:] - col[:HALF])], axis=1
    )
    w0 = (dot(k[:HALF], q, 1, 1) * decay).astype(BF16)
    g0 = (dot(v[:HALF], ga, 1, 1) * decay).astype(BF16)
    decay = triangle(row[:, HALF:], col[HALF:])
    w1 = (dot(k[HALF:], q[HALF:], 1, 1) * decay).astype(BF16)
    g1 = (dot(v[HALF:], ga[HALF:], 1, 1) * decay).astype(BF16)
    gk = jnp.concatenate([dot(g0, q, 1, 0), dot(g1, q[HALF:], 1, 0)], axis=0)
    gv = jnp.concatenate([dot(w0, ga, 1, 0), dot(w1, ga[HALF:], 1, 0)], axis=0)
    late_g = jnp.concatenate([g0[:, HALF:], g1], axis=0)
    gq = jnp.concatenate([dot(g0[:, :HALF], k[:HALF], 0, 0), dot(late_g, k, 0, 0)], axis=0)
    return gq, gk, gv


def forward_kernel(hp, n, start, cum_in, q_in, k_in, v_in, after_ref, *refs):
    out_hbm, turned_hbm, qd_hbm, kd_hbm, vd_hbm, mark_ref = refs[-19:-13]
    q_ref, k_ref, v_ref, out_ref, turned_ref, qd_ref, kd_ref, vd_ref = refs[-13:-5]
    cum_ref, cum_t_ref, cum_sem, in_sem, out_sem = refs[-5:]
    cum_copy = pltpu.make_async_copy(cum_in, cum_ref, cum_sem)
    cum_copy.start()
    mark_ref[...] = jnp.zeros_like(mark_ref)
    count = out_ref.shape[1] // DH
    into = ((q_in, q_ref), (k_in, k_ref), (v_in, v_ref))
    out = ((out_ref, out_hbm), (qd_ref, qd_hbm), (kd_ref, kd_hbm), (vd_ref, vd_hbm))

    def spots(step):
        return lanes_of(step * hp, hp), lanes_of(start + step * hp, hp)

    def arrive(step):
        near_at, far_at = spots(step)
        return [
            pltpu.make_async_copy(a.at[:, far_at], b.at[:, near_at], in_sem.at[j, step])
            for j, (a, b) in enumerate(into)
        ]

    def leave(step):
        near_at, far_at = spots(step)
        return [
            pltpu.make_async_copy(a.at[:, near_at], b.at[:, far_at], out_sem.at[j, step])
            for j, (a, b) in enumerate(out)
        ] + [
            pltpu.make_async_copy(
                turned_ref.at[near_at], turned_hbm.at[far_at], out_sem.at[len(out), step]
            )
        ]

    begin(arrive, count // hp)
    cum_copy.wait()
    cum_t_ref[...] = turn(cum_ref[...])

    def body(step, first):
        next_piece(arrive, step, count // hp)
        cols = columns(cum_t_ref, start + first)
        growth = jnp.exp(cols)
        tail = jnp.exp(cols[-1:, :] - cols)
        for i in range(hp):
            lanes = lanes_of(first + i)
            qd = (q_ref[:, lanes].astype(F32) * growth[:, i : i + 1]).astype(BF16)
            qd_ref[:, lanes] = qd
            turned_ref[lanes, :] = qd.T
            tail_i = jnp.broadcast_to(tail[:, i : i + 1], (tail.shape[0], DH))
            kd_ref[:, lanes] = (k_ref[:, lanes].astype(F32) * tail_i).astype(BF16)
            vd_ref[:, lanes] = (v_ref[:, lanes].astype(F32) * tail_i).astype(BF16)
            state = None
            base = jnp.zeros((1, 1), F32)
            for j in range(n):
                at = slice(j * CHUNK, (j + 1) * CHUNK)
                col = cols[at, i : i + 1]
                end = col[CHUNK - 1 :, :]
                row = cum_ref[pl.ds(start + first + i, 1), at]
                q, k, v = q_ref[at, lanes], k_ref[at, lanes], v_ref[at, lanes]
                a = attend(q, k, v, col, row)
                if j > 0:
                    a = a + jnp.exp(col - base) * dot(q, state.astype(BF16), 1, 0)
                out_ref[at, lanes] = a.astype(BF16)
                if j < n - 1:
                    new = dot(late(k, row, end), v, 1, 0)
                    state = new if state is None else state * jnp.exp(end - base) + new
                base = end
        for copy in leave(step):
            copy.start()

    over_heads(count, hp, body)
    for step in range(count // hp):
        for copy in leave(step):
            copy.wait()


def fetch_kernel(*refs):
    n = (len(refs) - 2) // 2
    sems = refs[-1]
    copies = [pltpu.make_async_copy(refs[i], refs[n + 1 + i], sems.at[i]) for i in range(n)]
    for copy in copies:
        copy.start()
    for copy in copies:
        copy.wait()


def sums_kernel(
    hp, core_ref, mine_ref, theirs_ref, gain_ref, q_ref, g_ref, a_ref, cum_in, sibling_in, turned_in,
    after_ref, att_ref, turned_ref, sum_ref, cum_ref, s_hbm,
    sq, cross, s_ref, sibling_ref, turned_sem, s_sem, sibling_sem, cum_sem,
):
    heads = s_ref.shape[0]
    beside_copy = pltpu.make_async_copy(sibling_in, sibling_ref, sibling_sem)
    beside_copy.start()
    core = core_ref[0]

    def assemble(h, carry):
        for half in range(2):
            s_ref[h, 64 * half : 64 * half + 64] = half_state(
                core, 2 * h + half, mine_ref, theirs_ref, sibling_ref, 1
            )
        return carry

    cum_copy = pltpu.make_async_copy(cum_in, cum_ref, cum_sem)
    cum_copy.start()
    beside_copy.wait()
    turned = pltpu.make_async_copy(turned_in, turned_ref, turned_sem)
    turned.start()
    lax.fori_loop(0, heads, assemble, 0)
    leave = pltpu.make_async_copy(s_ref, s_hbm, s_sem)
    leave.start()
    sq[...] = jnp.zeros_like(sq)
    cross[...] = jnp.zeros_like(cross)

    def body(step, first):
        sq_sum, cross_sum = sq[...], cross[...]
        for i in range(0, hp, 2):
            h = first + i
            lanes = lanes_of(h, 2)
            both = pair(s_ref[h].astype(BF16), s_ref[h + 1].astype(BF16))
            att = a_ref[:, lanes].astype(F32) + dot(q_ref[:, lanes], both, 1, 0)
            att_ref[:, lanes] = att
            gg = g_ref[:, lanes].astype(F32) * gain_ref[:, lanes]
            square, product = att * att, gg * att
            sq_sum = sq_sum + (square[:, :DH] + square[:, DH:])
            cross_sum = cross_sum + (product[:, :DH] + product[:, DH:])
        sq[...] = sq_sum
        cross[...] = cross_sum

    over_heads(heads, hp, body)
    a = jnp.sum(sq[...].T, axis=0, keepdims=True)
    b = jnp.sum(cross[...].T, axis=0, keepdims=True)
    which = lax.broadcasted_iota(jnp.int32, sum_ref.shape, 0)
    sum_ref[...] = jnp.where(which == 0, a, b)
    turned.wait()
    cum_copy.wait()
    leave.wait()


def grad_kernel(
    hp, cum_ref, turned_ref, g_ref, att_ref, gain_ref, s0, s1, s2, s3, state_ref, out_hbm, ga_hbm,
    inv_ref, both_ref, out_ref, ga_ref, out_sem,
):
    sums = (s0[...] + s1[...]) + (s2[...] + s3[...])
    inverse = lax.rsqrt(sums[0:1] / HD + EPSILON)
    center = sums[1:2] * inverse / HD
    both = inverse * inverse * center
    length = both.shape[1]
    inv_ref[...] = jnp.broadcast_to(inverse, (128, length)).T
    both_ref[...] = jnp.broadcast_to(both, (128, length)).T
    heads = state_ref.shape[0] // 2
    which = lax.broadcasted_iota(jnp.int32, (8, DH), 0)

    def leave(step):
        return (
            copy_piece(out_ref, out_hbm, out_sem.at[0], step, hp),
            copy_piece(ga_ref, ga_hbm, out_sem.at[1], step, hp),
        )

    def body(step, first):
        inverse, both = inv_ref[...], both_ref[...]
        for i in range(hp):
            lanes = lanes_of(first + i)
            att = att_ref[:, lanes]
            gain = gain_ref[:, lanes]
            scaled = g_ref[:, lanes].astype(F32) * inverse
            ga = (scaled * gain - both * att).astype(BF16)
            ga_ref[:, lanes] = ga
            out_ref[:, lanes] = (att * inverse * gain).astype(BF16)
            gain_part = jnp.sum(scaled * att, axis=0, keepdims=True)
            turned = turned_ref[pl.ds(pl.multiple_of((first + i) * DH, DH), DH), :]
            decay = jnp.exp(cum_ref[pl.ds(first + i, 1), :][:, -1:])
            extra = jnp.where(which == 0, gain_part, decay)
            send_state(state_ref, first + i, dot(turned, ga, 1, 0), extra)
        for copy in leave(step):
            copy.start()

    over_heads(heads, hp, body)
    for step in range(heads // hp):
        for copy in leave(step):
            copy.wait()


def backward_kernel(
    hp, n, start, cum_in, s_in, q_in, k_in, v_in, ga_in, after_ref, *refs
):
    gq_hbm, gk_hbm, gv_hbm, mark_ref = refs[-18:-14]
    q_ref, k_ref, v_ref, ga_ref, gq_ref, gk_ref, gv_ref = refs[-14:-7]
    cum_ref, s_ref, cum_t_ref, cum_sem, s_sem, in_sem, out_sem = refs[-7:]
    cum_copy = pltpu.make_async_copy(cum_in, cum_ref, cum_sem)
    cum_copy.start()
    mark_ref[...] = jnp.zeros_like(mark_ref)
    count = gk_ref.shape[1] // DH
    into = ((q_in, q_ref), (k_in, k_ref), (v_in, v_ref), (ga_in, ga_ref))
    out = ((gq_ref, gq_hbm), (gk_ref, gk_hbm), (gv_ref, gv_hbm))

    def spots(step):
        return lanes_of(step * hp, hp), lanes_of(start + step * hp, hp)

    def arrive(step):
        near_at, far_at = spots(step)
        return [
            pltpu.make_async_copy(a.at[:, far_at], b.at[:, near_at], in_sem.at[j, step])
            for j, (a, b) in enumerate(into)
        ] + [
            pltpu.make_async_copy(
                s_in.at[pl.ds(start + step * hp, hp)], s_ref.at[pl.ds(step * hp, hp)], s_sem.at[step]
            )
        ]

    def leave(step):
        near_at, far_at = spots(step)
        return [
            pltpu.make_async_copy(a.at[:, near_at], b.at[:, far_at], out_sem.at[j, step])
            for j, (a, b) in enumerate(out)
        ]

    begin(arrive, count // hp)
    cum_copy.wait()
    cum_t_ref[...] = turn(cum_ref[...])

    def body(step, first):
        next_piece(arrive, step, count // hp)
        cols = columns(cum_t_ref, start + first)
        for i in range(hp):
            h = start + first + i
            lanes = lanes_of(first + i)
            states = [s_ref[first + i]]
            ends = [jnp.zeros((1, 1), F32)]
            for j in range(n):
                at = slice(j * CHUNK, (j + 1) * CHUNK)
                col = cols[at, i : i + 1]
                end = col[CHUNK - 1 :, :]
                if j < n - 1:
                    row = cum_ref[pl.ds(h, 1), at]
                    kd = late(k_ref[at, lanes], row, end)
                    states.append(
                        states[-1] * jnp.exp(end - ends[-1]) + dot(kd, v_ref[at, lanes], 1, 0)
                    )
                ends.append(end)
            after = None
            for j in reversed(range(n)):
                at = slice(j * CHUNK, (j + 1) * CHUNK)
                col = cols[at, i : i + 1]
                row = cum_ref[pl.ds(h, 1), at]
                q, k, v = q_ref[at, lanes], k_ref[at, lanes], v_ref[at, lanes]
                ga = ga_ref[at, lanes]
                gq, gk, gv = attend_back(q, k, v, ga, col, row)
                gq = gq + jnp.exp(col - ends[j]) * dot(ga, states[j].astype(BF16), 1, 1)
                if after is not None:
                    tail = jnp.exp(ends[j + 1] - col)
                    low = after.astype(BF16)
                    gk = gk + tail * dot(v, low, 1, 1)
                    gv = gv + tail * dot(k, low, 1, 0)
                gq_ref[at, lanes] = gq.astype(BF16)
                gk_ref[at, lanes] = gk.astype(BF16)
                gv_ref[at, lanes] = gv.astype(BF16)
                if j > 0:
                    qd = (q.T.astype(F32) * jnp.exp(row - ends[j])).astype(BF16)
                    new = dot(qd, ga, 1, 0)
                    after = new if after is None else after * jnp.exp(ends[j + 1] - ends[j]) + new
        for copy in leave(step):
            copy.start()

    over_heads(count, hp, body)
    for step in range(count // hp):
        for copy in leave(step):
            copy.wait()


def final_kernel(
    hp, state_ref, k_in, v_in, gk_in, gv_in, after_ref, gk_hbm, gv_hbm, gain_ref,
    k_ref, v_ref, gk_ref, gv_ref, in_sem, out_sem,
):
    into = ((k_in, k_ref), (v_in, v_ref), (gk_in, gk_ref), (gv_in, gv_ref))
    heads = state_ref.shape[0] // 2

    def arrive(step):
        return [copy_piece(a, b, in_sem.at[j], step, hp) for j, (a, b) in enumerate(into)]

    def leave(step):
        return (
            copy_piece(gk_ref, gk_hbm, out_sem.at[0], step, hp),
            copy_piece(gv_ref, gv_hbm, out_sem.at[1], step, hp),
        )

    for i in range(heads // hp):
        for copy in arrive(i):
            copy.start()

    def body(step, first):
        for copy in arrive(step):
            copy.wait()
        for i in range(0, hp, 2):
            h = first + i
            lanes = lanes_of(h, 2)
            states = []
            for j in (h, h + 1):
                halves = [state_ref[2 * j, 0:64], state_ref[2 * j + 1, 0:64]]
                gain_ref[:, lanes_of(j)] = state_ref[2 * j, 64:65]
                states.append(jnp.concatenate(halves, axis=0).astype(BF16))
            both = pair(*states)
            gk_ref[:, lanes] = (
                gk_ref[:, lanes].astype(F32) + dot(v_ref[:, lanes], both, 1, 1)
            ).astype(BF16)
            gv_ref[:, lanes] = (
                gv_ref[:, lanes].astype(F32) + dot(k_ref[:, lanes], both, 1, 0)
            ).astype(BF16)
        for copy in leave(step):
            copy.start()

    over_heads(heads, hp, body)
    for step in range(heads // hp):
        for copy in leave(step):
            copy.wait()


def by_core(core, mine, theirs):
    return jnp.where(core == 0, mine, theirs), jnp.where(core == 0, theirs, mine)


def combine_forward_kernel(core_ref, mine_ref, theirs_ref, out_ref):
    core = core_ref[0]
    n = out_ref.shape[0]
    for i in range(n):
        at = core * n + i
        first, second = by_core(core, mine_ref[at], theirs_ref[at])
        decay = second[64:65]
        out_ref[i, 0:64] = first[0:64] * decay + second[0:64]
        out_ref[i, 64:72] = first[64:72] * second[64:72]


def scan_forward_kernel(x_ref, mark_ref, out_ref):
    n = x_ref.shape[0]
    state = jnp.zeros((64, 128), F32)
    for j in range(n):
        out_ref[j] = state
        if j < n - 1:
            state = state * x_ref[j, 64:65] + x_ref[j, 0:64]


def scan_backward_kernel(x_ref, mark_ref, out_ref):
    n = x_ref.shape[0]
    state = jnp.zeros((64, 128), F32)
    gain = jnp.zeros((8, 128), F32)
    for j in reversed(range(n)):
        out_ref[j, 0:64] = state
        state = state * x_ref[j, 65:66] + x_ref[j, 0:64]
        gain = gain + x_ref[j, 64:72]
    for j in range(n):
        out_ref[j, 64:72] = gain


def half_state(core, m, mine_ref, theirs_ref, sibling_ref, last):
    n = mine_ref.shape[0]
    here = core * n
    own = (m >= here) & (m < here + n)
    at = lax.rem(m, n)
    value = jnp.where(own, mine_ref[at, 0:64], theirs_ref[at, 0:64])
    beside = sibling_ref[m]
    return jnp.where(core == last, value * beside[64:65] + beside[0:64], value)


def cost(flops, moved, exps=0):
    return pl.CostEstimate(flops=int(flops), bytes_accessed=int(moved), transcendentals=int(exps))


def far(x):
    return pltpu.with_memory_space_constraint(x, pltpu.HBM)


def near(x):
    return pltpu.with_memory_space_constraint(x, pltpu.VMEM)


def exchange(x, axes):
    return lax.all_to_all(x, axes, split_axis=0, concat_axis=0, tiled=True)


def beside(x):
    return lax.ppermute(x, SEQ[2], [(0, 1), (1, 0)])


def other_heads(sums):
    groups = lax.axis_size("head")
    return [
        lax.ppermute(sums, "head", [(i, (i + shift) % groups) for i in range(groups)])
        for shift in range(1, groups)
    ]


def on_device(queries, key_rows, value_rows, log_decay, norm_gain, grad_out):
    tokens, width = queries.shape
    heads = width // DH
    devices = 2 * heads
    chunks = tokens // CHUNK
    gain = norm_gain[None, :]
    rows = (tokens, width)
    flat = pltpu.HBM(rows, BF16)
    kept = pltpu.VMEM(rows, BF16)
    sent = pltpu.HBM((devices, 72, DH), F32)
    joined = pltpu.HBM((devices // 2, 72, DH), F32)
    core = lax.axis_index(SEQ[2])[None].astype(jnp.int32)
    scalar = pl.BlockSpec(memory_space=pltpu.SMEM)
    here = pl.BlockSpec(memory_space=pltpu.VMEM)
    there = pl.BlockSpec(memory_space=pl.ANY)
    settings = pltpu.CompilerParams(vmem_limit_bytes=LIMIT)
    queries, key_rows, value_rows, grad_out = map(far, (queries, key_rows, value_rows, grad_out))

    def sems(*n):
        return pltpu.SemaphoreType.DMA(n)

    hp = 4
    local, cum = pl.pallas_call(
        functools.partial(local_kernel, hp),
        in_specs=[here, there, there],
        out_specs=[here] * 2,
        out_shape=[pltpu.VMEM(sent.shape, F32), pltpu.HBM((heads, tokens), F32)],
        scratch_shapes=[kept] * 2 + [sems(heads // hp)] * 2,
        compiler_params=settings,
        name="local_state",
    )(far(log_decay), key_rows, value_rows)
    cum = far(cum)

    mark_shape = pltpu.HBM((8, 128), F32)
    cum_t_shape = pltpu.VMEM((tokens, 128), F32)
    cum_shape = pltpu.VMEM((heads, tokens), F32)
    one_sem = pltpu.SemaphoreType.DMA

    def forward_part(start, count, after, ready):
        hp = 2
        part = pltpu.VMEM((tokens, count * DH), BF16)
        part_t = pltpu.VMEM((count * DH, tokens), BF16)
        *ready, mark = pl.pallas_call(
            functools.partial(forward_kernel, hp, chunks, start),
            in_specs=[there] * (5 + len(ready)),
            out_specs=[there] * 5 + [here],
            out_shape=[flat, pltpu.HBM((width, tokens), BF16), flat, flat, flat, mark_shape],
            scratch_shapes=[part] * 4
            + [part_t]
            + [part] * 3
            + [cum_shape, cum_t_shape, one_sem, sems(3, count // hp), sems(5, count // hp)],
            input_output_aliases={5 + i: i for i in range(len(ready))},
            compiler_params=settings,
            cost_estimate=cost(8e9, 13e6, 3e6),
            name="forward_intra",
        )(cum, queries, key_rows, value_rows, far(after), *map(far, ready))
        return ready, far(mark)

    def backward_part(start, count, after, ready):
        hp = 2
        part = pltpu.VMEM((tokens, count * DH), BF16)
        *ready, mark = pl.pallas_call(
            functools.partial(backward_kernel, hp, chunks, start),
            in_specs=[there] * (7 + len(ready)),
            out_specs=[there] * 3 + [here],
            out_shape=[flat] * 3 + [mark_shape],
            scratch_shapes=[part] * 7
            + [cum_shape, pltpu.VMEM((count, DH, DH), F32), cum_t_shape, one_sem]
            + [sems(count // hp), sems(4, count // hp), sems(3, count // hp)],
            input_output_aliases={7 + i: i for i in range(len(ready))},
            compiler_params=settings,
            cost_estimate=cost(10e9, 15e6, 2e6),
            name="backward_intra",
        )(
            cum, far(state_in), queries, key_rows, value_rows, far(grad_attended), far(after),
            *map(far, ready),
        )
        return ready, far(mark)

    def travel(chip, axes, scan, part, counts):
        got = exchange(chip, axes)
        ready, mark = part(0, counts[0], chip, [])
        passed = scan(got, mark)
        edge = exchange(passed, axes)
        ready, mark = part(counts[0], counts[1], passed, ready)
        edge, last = lax.optimization_barrier((edge, mark))
        return edge, far(last), ready

    sibling = beside(near(local))
    chip = pl.pallas_call(
        combine_forward_kernel,
        in_specs=[scalar, here, here],
        out_specs=here,
        out_shape=joined,
        compiler_params=settings,
        name="combine_forward",
    )(core, near(local), near(sibling))

    def scan_forward(got, mark):
        return pl.pallas_call(
            scan_forward_kernel,
            in_specs=[here, there],
            out_specs=here,
            out_shape=pltpu.HBM((devices // 2, 64, DH), F32),
            compiler_params=settings,
            name="scan_forward",
        )(got, mark)

    chip_state, last, ready = travel(chip, SEQ[:2], scan_forward, forward_part, FORWARD_CUTS)
    sibling_state = beside(chip_state)
    attended_local, turned, grown, faded_k, faded_v = map(far, ready)

    grown, grads, attended_local = pl.pallas_call(
        fetch_kernel,
        in_specs=[there] * 4,
        out_specs=[here] * 3,
        out_shape=[kept] * 3,
        scratch_shapes=[sems(3)],
        compiler_params=settings,
        cost_estimate=cost(1e9, 19e6),
        name="fetch_rows",
    )(grown, grad_out, attended_local, chip_state)

    hp = 2
    attended, turned, sums, cum_here, state_in = pl.pallas_call(
        functools.partial(sums_kernel, hp),
        in_specs=[scalar] + [here] * 6 + [there] * 4,
        out_specs=[here] * 4 + [there],
        out_shape=[
            pltpu.VMEM(rows, F32),
            pltpu.VMEM((width, tokens), BF16),
            pltpu.VMEM((8, tokens), F32),
            pltpu.VMEM((heads, tokens), F32),
            pltpu.HBM((heads, DH, DH), F32),
        ],
        scratch_shapes=[pltpu.VMEM((tokens, 128), F32)] * 2
        + [pltpu.VMEM((heads, DH, DH), F32), pltpu.VMEM((devices, 72, DH), F32)]
        + [pltpu.SemaphoreType.DMA] * 4,
        compiler_params=settings,
        name="row_sums",
    )(
        core, chip_state, near(sibling_state), gain, near(grown), near(grads), near(attended_local),
        cum, far(sibling), turned, last,
    )

    hp = 4
    others = other_heads(sums)
    sent_grad, output, grad_attended = pl.pallas_call(
        functools.partial(grad_kernel, hp),
        in_specs=[here] * 9,
        out_specs=[here] + [there] * 2,
        out_shape=[sent, flat, flat],
        scratch_shapes=[pltpu.VMEM((tokens, 128), F32)] * 2 + [kept] * 2 + [sems(2, heads // hp)],
        compiler_params=settings,
        name="grad_state",
    )(near(cum_here), near(turned), near(grads), near(attended), gain, *map(near, (sums, *others)))

    def scan_backward(got_grad, mark):
        return pl.pallas_call(
            scan_backward_kernel,
            in_specs=[here, there],
            out_specs=here,
            out_shape=sent,
            compiler_params=settings,
            name="scan_backward",
        )(got_grad, mark)

    back, last_grad, ready = travel(sent_grad, SEQ, scan_backward, backward_part, BACKWARD_CUTS)
    grad_q, part_k, part_v = ready

    hp = 2
    grad_k, grad_v, grad_gain = pl.pallas_call(
        functools.partial(final_kernel, hp),
        in_specs=[here] + [there] * 5,
        out_specs=[there] * 2 + [here],
        out_shape=[flat] * 2 + [jax.ShapeDtypeStruct((1, width), F32)],
        scratch_shapes=[kept] * 4
        + [sems(4, heads // hp), sems(2, heads // hp)],
        compiler_params=settings,
        name="final_grads",
    )(near(back), faded_k, faded_v, far(part_k), far(part_v), last_grad)
    return output, grad_q, grad_k, grad_v, grad_gain.reshape(width)


def solution(mesh):
    split = Mesh(
        mesh.devices.reshape(4, 4, 2, mesh.shape["head"]), ("seq_0", "seq_1", "seq_2", "head")
    )
    placed = (
        P(SEQ, "head"),
        P(SEQ, "head"),
        P(SEQ, "head"),
        P("head", SEQ),
        P("head"),
        P(SEQ, "head"),
    )
    return jax.shard_map(
        on_device,
        mesh=split,
        in_specs=placed,
        out_specs=(P(SEQ, "head"), P(SEQ, "head"), P(SEQ, "head"), P(SEQ, "head"), P("head")),
        check_vma=False,
    )
```

```python
import functools

import jax
import jax.numpy as jnp
from jax import lax
from jax.experimental import pallas as pl
from jax.experimental.pallas import tpu as pltpu
from jax.sharding import Mesh
from jax.sharding import PartitionSpec as P

DH = 128
HD = 8192
EPSILON = 1e-06
CHUNK = 256
HALF = CHUNK // 2
LIMIT = 28 * 10**6
FORWARD_CUTS = (8, 8)
BACKWARD_CUTS = (8, 8)
SEQ = ("seq_0", "seq_1", "seq_2")
F32 = jnp.float32
BF16 = jnp.bfloat16


def dot(a, b, ca, cb, precision=None):
    return lax.dot_general(
        a, b, (((ca,), (cb,)), ((), ())), precision=precision, preferred_element_type=F32
    )


def lane_prefix(x):
    rows, n = x.shape
    high = x.astype(BF16)
    rest = x - high.astype(F32)
    middle = rest.astype(BF16)
    low = (rest - middle.astype(F32)).astype(BF16)
    blocks = n // 128
    parts = [p[:, 128 * b : 128 * b + 128] for b in range(blocks) for p in (high, middle, low)]
    stacked = jnp.concatenate(parts, axis=0)
    s = lax.broadcasted_iota(jnp.int32, (128, 128), 0)
    t = lax.broadcasted_iota(jnp.int32, (128, 128), 1)
    sums = dot(stacked, (s <= t).astype(BF16), 1, 0)
    out, before = [], jnp.zeros((rows, 1), F32)
    for b in range(blocks):
        first = 3 * rows * b
        inside = (
            sums[first : first + rows]
            + (sums[first + rows : first + 2 * rows] + sums[first + 2 * rows : first + 3 * rows])
        )
        out.append(inside + before)
        before = out[-1][:, 127:]
    return jnp.concatenate(out, axis=1)


def turn(rows_of):
    heads, n = rows_of.shape
    return jnp.concatenate([rows_of, jnp.zeros((128 - heads, n), F32)], axis=0).T


def columns(cum_t_ref, first):
    return pltpu.roll(cum_t_ref[...], lax.rem(128 - first, 128), 1)


def pair(first, second):
    zero = jnp.zeros_like(first)
    return jnp.concatenate(
        [jnp.concatenate([first, zero], axis=1), jnp.concatenate([zero, second], axis=1)], axis=0
    )


def lanes_of(h, n=1):
    return pl.ds(pl.multiple_of(h * DH, DH), n * DH)


def over_heads(count, step, body):
    lax.fori_loop(0, count // step, lambda i, c: (body(i, i * step), c)[1], 0)


AHEAD = 2


def begin(arrive, steps):
    for i in range(min(AHEAD, steps)):
        for copy in arrive(i):
            copy.start()


def next_piece(arrive, step, steps):
    for copy in arrive(step):
        copy.wait()

    @pl.when(step + AHEAD < steps)
    def _():
        for copy in arrive(step + AHEAD):
            copy.start()


def copy_piece(source, target, sems, i, n):
    at = lanes_of(i * n, n)
    return pltpu.make_async_copy(source.at[:, at], target.at[:, at], sems.at[i])


def send_state(state_ref, h, s, extra):
    for half in range(2):
        state_ref[2 * h + half, 0:64] = s[64 * half : 64 * half + 64]
        state_ref[2 * h + half, 64:72] = jnp.broadcast_to(extra, (8, 128))


def local_kernel(hp, ld_ref, k_in, v_in, state_ref, cum_ref, k_ref, v_ref, k_sem, v_sem):
    heads = ld_ref.shape[0]

    def arrive(i):
        return copy_piece(k_in, k_ref, k_sem, i, hp), copy_piece(v_in, v_ref, v_sem, i, hp)

    begin(arrive, heads // hp)
    cum_ref[...] = lane_prefix(ld_ref[...])

    def body(i, first):
        next_piece(arrive, i, heads // hp)
        for j in range(hp):
            at = lanes_of(first + j)
            row = cum_ref[pl.ds(first + j, 1), :]
            end = row[:, -1:]
            k = late(k_ref[:, at], row, end)
            send_state(state_ref, first + j, dot(k, v_ref[:, at], 1, 0), jnp.exp(end))

    over_heads(heads, hp, body)


def late(k, row, end):
    return (k.T.astype(F32) * jnp.exp(end - row)).astype(BF16)


def triangle(row, col):
    s = lax.broadcasted_iota(jnp.int32, (HALF, HALF), 0)
    t = lax.broadcasted_iota(jnp.int32, (HALF, HALF), 1)
    return jnp.where(s <= t, jnp.exp(row - col), 0.0)


def attend(q, k, v, col, row):
    t = lax.broadcasted_iota(jnp.int32, (CHUNK, CHUNK), 0)
    s = lax.broadcasted_iota(jnp.int32, (CHUNK, CHUNK), 1)
    decay = jnp.where(t >= s, jnp.exp(col - row), 0.0)
    return dot((dot(q, k, 1, 1) * decay).astype(BF16), v, 1, 0)


def attend_back(q, k, v, ga, col, row):
    decay = jnp.concatenate(
        [triangle(row[:, :HALF], col[:HALF]), jnp.exp(row[:, HALF:] - col[:HALF])], axis=1
    )
    w0 = (dot(k[:HALF], q, 1, 1) * decay).astype(BF16)
    g0 = (dot(v[:HALF], ga, 1, 1) * decay).astype(BF16)
    decay = triangle(row[:, HALF:], col[HALF:])
    w1 = (dot(k[HALF:], q[HALF:], 1, 1) * decay).astype(BF16)
    g1 = (dot(v[HALF:], ga[HALF:], 1, 1) * decay).astype(BF16)
    gk = jnp.concatenate([dot(g0, q, 1, 0), dot(g1, q[HALF:], 1, 0)], axis=0)
    gv = jnp.concatenate([dot(w0, ga, 1, 0), dot(w1, ga[HALF:], 1, 0)], axis=0)
    late_g = jnp.concatenate([g0[:, HALF:], g1], axis=0)
    gq = jnp.concatenate([dot(g0[:, :HALF], k[:HALF], 0, 0), dot(late_g, k, 0, 0)], axis=0)
    return gq, gk, gv


def forward_kernel(hp, n, start, cum_in, q_in, k_in, v_in, after_ref, *refs):
    out_hbm, turned_hbm, qd_hbm, kd_hbm, vd_hbm, mark_ref = refs[-19:-13]
    q_ref, k_ref, v_ref, out_ref, turned_ref, qd_ref, kd_ref, vd_ref = refs[-13:-5]
    cum_ref, cum_t_ref, cum_sem, in_sem, out_sem = refs[-5:]
    cum_copy = pltpu.make_async_copy(cum_in, cum_ref, cum_sem)
    cum_copy.start()
    mark_ref[...] = jnp.zeros_like(mark_ref)
    count = out_ref.shape[1] // DH
    into = ((q_in, q_ref), (k_in, k_ref), (v_in, v_ref))
    out = ((out_ref, out_hbm), (qd_ref, qd_hbm), (kd_ref, kd_hbm), (vd_ref, vd_hbm))

    def spots(step):
        return lanes_of(step * hp, hp), lanes_of(start + step * hp, hp)

    def arrive(step):
        near_at, far_at = spots(step)
        return [
            pltpu.make_async_copy(a.at[:, far_at], b.at[:, near_at], in_sem.at[j, step])
            for j, (a, b) in enumerate(into)
        ]

    def leave(step):
        near_at, far_at = spots(step)
        return [
            pltpu.make_async_copy(a.at[:, near_at], b.at[:, far_at], out_sem.at[j, step])
            for j, (a, b) in enumerate(out)
        ] + [
            pltpu.make_async_copy(
                turned_ref.at[near_at], turned_hbm.at[far_at], out_sem.at[len(out), step]
            )
        ]

    begin(arrive, count // hp)
    cum_copy.wait()
    cum_t_ref[...] = turn(cum_ref[...])

    def body(step, first):
        next_piece(arrive, step, count // hp)
        cols = columns(cum_t_ref, start + first)
        growth = jnp.exp(cols)
        tail = jnp.exp(cols[-1:, :] - cols)
        for i in range(hp):
            lanes = lanes_of(first + i)
            qd = (q_ref[:, lanes].astype(F32) * growth[:, i : i + 1]).astype(BF16)
            qd_ref[:, lanes] = qd
            turned_ref[lanes, :] = qd.T
            tail_i = jnp.broadcast_to(tail[:, i : i + 1], (tail.shape[0], DH))
            kd_ref[:, lanes] = (k_ref[:, lanes].astype(F32) * tail_i).astype(BF16)
            vd_ref[:, lanes] = (v_ref[:, lanes].astype(F32) * tail_i).astype(BF16)
            state = None
            base = jnp.zeros((1, 1), F32)
            for j in range(n):
                at = slice(j * CHUNK, (j + 1) * CHUNK)
                col = cols[at, i : i + 1]
                end = col[CHUNK - 1 :, :]
                row = cum_ref[pl.ds(start + first + i, 1), at]
                q, k, v = q_ref[at, lanes], k_ref[at, lanes], v_ref[at, lanes]
                a = attend(q, k, v, col, row)
                if j > 0:
                    a = a + jnp.exp(col - base) * dot(q, state.astype(BF16), 1, 0)
                out_ref[at, lanes] = a.astype(BF16)
                if j < n - 1:
                    new = dot(late(k, row, end), v, 1, 0)
                    state = new if state is None else state * jnp.exp(end - base) + new
                base = end
        for copy in leave(step):
            copy.start()

    over_heads(count, hp, body)
    for step in range(count // hp):
        for copy in leave(step):
            copy.wait()


def fetch_kernel(*refs):
    n = (len(refs) - 2) // 2
    sems = refs[-1]
    copies = [pltpu.make_async_copy(refs[i], refs[n + 1 + i], sems.at[i]) for i in range(n)]
    for copy in copies:
        copy.start()
    for copy in copies:
        copy.wait()


def sums_kernel(
    hp, core_ref, mine_ref, theirs_ref, gain_ref, q_ref, a_ref, sibling_ref, g_in, cum_in, turned_in,
    after_ref, att_ref, g_ref, turned_ref, sum_ref, cum_ref, s_hbm,
    sq, cross, s_ref, g_sem, turned_sem, s_sem, cum_sem,
):
    heads = s_ref.shape[0]
    for i in range(heads // hp):
        copy_piece(g_in, g_ref, g_sem, i, hp).start()
    core = core_ref[0]

    def assemble(h, carry):
        for half in range(2):
            s_ref[h, 64 * half : 64 * half + 64] = half_state(
                core, 2 * h + half, mine_ref, theirs_ref, sibling_ref, 1, 64
            )
        return carry

    cum_copy = pltpu.make_async_copy(cum_in, cum_ref, cum_sem)
    cum_copy.start()
    turned = pltpu.make_async_copy(turned_in, turned_ref, turned_sem)
    turned.start()
    lax.fori_loop(0, heads, assemble, 0)
    leave = pltpu.make_async_copy(s_ref, s_hbm, s_sem)
    leave.start()
    sq[...] = jnp.zeros_like(sq)
    cross[...] = jnp.zeros_like(cross)

    def body(step, first):
        copy_piece(g_in, g_ref, g_sem, step, hp).wait()
        sq_sum, cross_sum = sq[...], cross[...]
        for i in range(0, hp, 2):
            h = first + i
            lanes = lanes_of(h, 2)
            both = pair(s_ref[h].astype(BF16), s_ref[h + 1].astype(BF16))
            att = a_ref[:, lanes].astype(F32) + dot(q_ref[:, lanes], both, 1, 0)
            att_ref[:, lanes] = att
            gg = g_ref[:, lanes].astype(F32) * gain_ref[:, lanes]
            square, product = att * att, gg * att
            sq_sum = sq_sum + (square[:, :DH] + square[:, DH:])
            cross_sum = cross_sum + (product[:, :DH] + product[:, DH:])
        sq[...] = sq_sum
        cross[...] = cross_sum

    over_heads(heads, hp, body)
    a = jnp.sum(sq[...].T, axis=0, keepdims=True)
    b = jnp.sum(cross[...].T, axis=0, keepdims=True)
    which = lax.broadcasted_iota(jnp.int32, sum_ref.shape, 0)
    sum_ref[...] = jnp.where(which == 0, a, b)
    turned.wait()
    cum_copy.wait()
    leave.wait()


def grad_kernel(
    hp, cum_ref, turned_ref, g_ref, att_ref, gain_ref, s0, s1, s2, s3, state_ref, out_hbm, ga_hbm,
    inv_ref, both_ref, out_ref, ga_ref, out_sem,
):
    sums = (s0[...] + s1[...]) + (s2[...] + s3[...])
    inverse = lax.rsqrt(sums[0:1] / HD + EPSILON)
    center = sums[1:2] * inverse / HD
    both = inverse * inverse * center
    length = both.shape[1]
    inv_ref[...] = jnp.broadcast_to(inverse, (128, length)).T
    both_ref[...] = jnp.broadcast_to(both, (128, length)).T
    heads = state_ref.shape[0] // 2
    which = lax.broadcasted_iota(jnp.int32, (8, DH), 0)

    def leave(step):
        return (
            copy_piece(out_ref, out_hbm, out_sem.at[0], step, hp),
            copy_piece(ga_ref, ga_hbm, out_sem.at[1], step, hp),
        )

    def body(step, first):
        inverse, both = inv_ref[...], both_ref[...]
        for i in range(hp):
            lanes = lanes_of(first + i)
            att = att_ref[:, lanes]
            gain = gain_ref[:, lanes]
            scaled = g_ref[:, lanes].astype(F32) * inverse
            ga = (scaled * gain - both * att).astype(BF16)
            ga_ref[:, lanes] = ga
            out_ref[:, lanes] = (att * inverse * gain).astype(BF16)
            gain_part = jnp.sum(scaled * att, axis=0, keepdims=True)
            turned = turned_ref[pl.ds(pl.multiple_of((first + i) * DH, DH), DH), :]
            decay = jnp.exp(cum_ref[pl.ds(first + i, 1), :][:, -1:])
            extra = jnp.where(which == 0, gain_part, decay)
            send_state(state_ref, first + i, dot(turned, ga, 1, 0), extra)
        for copy in leave(step):
            copy.start()

    over_heads(heads, hp, body)
    for step in range(heads // hp):
        for copy in leave(step):
            copy.wait()


def backward_kernel(
    hp, n, start, cum_in, s_in, q_in, k_in, v_in, ga_in, after_ref, *refs
):
    gq_hbm, gk_hbm, gv_hbm, mark_ref = refs[-18:-14]
    q_ref, k_ref, v_ref, ga_ref, gq_ref, gk_ref, gv_ref = refs[-14:-7]
    cum_ref, s_ref, cum_t_ref, cum_sem, s_sem, in_sem, out_sem = refs[-7:]
    cum_copy = pltpu.make_async_copy(cum_in, cum_ref, cum_sem)
    cum_copy.start()
    mark_ref[...] = jnp.zeros_like(mark_ref)
    count = gk_ref.shape[1] // DH
    into = ((q_in, q_ref), (k_in, k_ref), (v_in, v_ref), (ga_in, ga_ref))
    out = ((gq_ref, gq_hbm), (gk_ref, gk_hbm), (gv_ref, gv_hbm))

    def spots(step):
        return lanes_of(step * hp, hp), lanes_of(start + step * hp, hp)

    def arrive(step):
        near_at, far_at = spots(step)
        return [
            pltpu.make_async_copy(a.at[:, far_at], b.at[:, near_at], in_sem.at[j, step])
            for j, (a, b) in enumerate(into)
        ] + [
            pltpu.make_async_copy(
                s_in.at[pl.ds(start + step * hp, hp)], s_ref.at[pl.ds(step * hp, hp)], s_sem.at[step]
            )
        ]

    def leave(step):
        near_at, far_at = spots(step)
        return [
            pltpu.make_async_copy(a.at[:, near_at], b.at[:, far_at], out_sem.at[j, step])
            for j, (a, b) in enumerate(out)
        ]

    begin(arrive, count // hp)
    cum_copy.wait()
    cum_t_ref[...] = turn(cum_ref[...])

    def body(step, first):
        next_piece(arrive, step, count // hp)
        cols = columns(cum_t_ref, start + first)
        for i in range(hp):
            h = start + first + i
            lanes = lanes_of(first + i)
            states = [s_ref[first + i]]
            ends = [jnp.zeros((1, 1), F32)]
            for j in range(n):
                at = slice(j * CHUNK, (j + 1) * CHUNK)
                col = cols[at, i : i + 1]
                end = col[CHUNK - 1 :, :]
                if j < n - 1:
                    row = cum_ref[pl.ds(h, 1), at]
                    kd = late(k_ref[at, lanes], row, end)
                    states.append(
                        states[-1] * jnp.exp(end - ends[-1]) + dot(kd, v_ref[at, lanes], 1, 0)
                    )
                ends.append(end)
            after = None
            for j in reversed(range(n)):
                at = slice(j * CHUNK, (j + 1) * CHUNK)
                col = cols[at, i : i + 1]
                row = cum_ref[pl.ds(h, 1), at]
                q, k, v = q_ref[at, lanes], k_ref[at, lanes], v_ref[at, lanes]
                ga = ga_ref[at, lanes]
                gq, gk, gv = attend_back(q, k, v, ga, col, row)
                gq = gq + jnp.exp(col - ends[j]) * dot(ga, states[j].astype(BF16), 1, 1)
                if after is not None:
                    tail = jnp.exp(ends[j + 1] - col)
                    low = after.astype(BF16)
                    gk = gk + tail * dot(v, low, 1, 1)
                    gv = gv + tail * dot(k, low, 1, 0)
                gq_ref[at, lanes] = gq.astype(BF16)
                gk_ref[at, lanes] = gk.astype(BF16)
                gv_ref[at, lanes] = gv.astype(BF16)
                if j > 0:
                    qd = (q.T.astype(F32) * jnp.exp(row - ends[j])).astype(BF16)
                    new = dot(qd, ga, 1, 0)
                    after = new if after is None else after * jnp.exp(ends[j + 1] - ends[j]) + new
        for copy in leave(step):
            copy.start()

    over_heads(count, hp, body)
    for step in range(count // hp):
        for copy in leave(step):
            copy.wait()


def final_kernel(
    hp, core_ref, mine_ref, theirs_ref, k_ref, v_ref, sibling_ref, gk_in, gv_in, after_ref,
    gk_hbm, gv_hbm, gain_ref, gk_ref, gv_ref, in_sem, out_sem,
):
    core = core_ref[0]
    into = ((gk_in, gk_ref), (gv_in, gv_ref))
    heads = sibling_ref.shape[0] // 2

    def arrive(step):
        return [copy_piece(a, b, in_sem.at[j], step, hp) for j, (a, b) in enumerate(into)]

    def leave(step):
        return (
            copy_piece(gk_ref, gk_hbm, out_sem.at[0], step, hp),
            copy_piece(gv_ref, gv_hbm, out_sem.at[1], step, hp),
        )

    for i in range(heads // hp):
        for copy in arrive(i):
            copy.start()

    def body(step, first):
        for copy in arrive(step):
            copy.wait()
        for i in range(0, hp, 2):
            h = first + i
            lanes = lanes_of(h, 2)
            states = []
            for j in (h, h + 1):
                halves = [
                    half_state(core, m, mine_ref, theirs_ref, sibling_ref, 0, 65)
                    for m in (2 * j, 2 * j + 1)
                ]
                n = mine_ref.shape[0]
                own = (2 * j >= core * n) & (2 * j < core * n + n)
                at = lax.rem(2 * j, n)
                gain_ref[:, lanes_of(j)] = jnp.where(
                    own, mine_ref[at, 64:65], theirs_ref[at, 64:65]
                )
                states.append(jnp.concatenate(halves, axis=0).astype(BF16))
            both = pair(*states)
            gk_ref[:, lanes] = (
                gk_ref[:, lanes].astype(F32) + dot(v_ref[:, lanes], both, 1, 1)
            ).astype(BF16)
            gv_ref[:, lanes] = (
                gv_ref[:, lanes].astype(F32) + dot(k_ref[:, lanes], both, 1, 0)
            ).astype(BF16)
        for copy in leave(step):
            copy.start()

    over_heads(heads, hp, body)
    for step in range(heads // hp):
        for copy in leave(step):
            copy.wait()


def by_core(core, mine, theirs):
    return jnp.where(core == 0, mine, theirs), jnp.where(core == 0, theirs, mine)


def combine_forward_kernel(core_ref, mine_ref, theirs_ref, out_ref):
    core = core_ref[0]
    n = out_ref.shape[0]
    for i in range(n):
        at = core * n + i
        first, second = by_core(core, mine_ref[at], theirs_ref[at])
        decay = second[64:65]
        out_ref[i, 0:64] = first[0:64] * decay + second[0:64]
        out_ref[i, 64:72] = first[64:72] * second[64:72]


def combine_backward_kernel(core_ref, mine_ref, theirs_ref, out_ref):
    core = core_ref[0]
    n = out_ref.shape[0]
    which = lax.broadcasted_iota(jnp.int32, (8, DH), 0)
    for i in range(n):
        at = core * n + i
        first, second = by_core(core, mine_ref[at], theirs_ref[at])
        out_ref[i, 0:64] = second[0:64] * first[65:66] + first[0:64]
        out_ref[i, 64:72] = jnp.where(
            which == 0, first[64:72] + second[64:72], first[64:72] * second[64:72]
        )


def scan_forward_kernel(x_ref, mark_ref, out_ref):
    n = x_ref.shape[0]
    state = jnp.zeros((64, 128), F32)
    for j in range(n):
        out_ref[j] = state
        if j < n - 1:
            state = state * x_ref[j, 64:65] + x_ref[j, 0:64]


def scan_backward_kernel(x_ref, mark_ref, out_ref):
    n = x_ref.shape[0]
    state = jnp.zeros((64, 128), F32)
    gain = jnp.zeros((8, 128), F32)
    for j in reversed(range(n)):
        out_ref[j, 0:64] = state
        state = state * x_ref[j, 65:66] + x_ref[j, 0:64]
        gain = gain + x_ref[j, 64:72]
    for j in range(n):
        out_ref[j, 64:72] = gain


def half_state(core, m, mine_ref, theirs_ref, sibling_ref, last, row):
    n = mine_ref.shape[0]
    here = core * n
    own = (m >= here) & (m < here + n)
    at = lax.rem(m, n)
    value = jnp.where(own, mine_ref[at, 0:64], theirs_ref[at, 0:64])
    beside = sibling_ref[m]
    return jnp.where(core == last, value * beside[row : row + 1] + beside[0:64], value)


def cost(flops, moved, exps=0):
    return pl.CostEstimate(flops=int(flops), bytes_accessed=int(moved), transcendentals=int(exps))


def far(x):
    return pltpu.with_memory_space_constraint(x, pltpu.HBM)


def near(x):
    return pltpu.with_memory_space_constraint(x, pltpu.VMEM)


def exchange(x, axes):
    return lax.all_to_all(x, axes, split_axis=0, concat_axis=0, tiled=True)


def beside(x):
    return lax.ppermute(x, SEQ[2], [(0, 1), (1, 0)])


def other_heads(sums):
    groups = lax.axis_size("head")
    return [
        lax.ppermute(sums, "head", [(i, (i + shift) % groups) for i in range(groups)])
        for shift in range(1, groups)
    ]


def on_device(queries, key_rows, value_rows, log_decay, norm_gain, grad_out):
    tokens, width = queries.shape
    heads = width // DH
    devices = 2 * heads
    chunks = tokens // CHUNK
    gain = norm_gain[None, :]
    rows = (tokens, width)
    flat = pltpu.HBM(rows, BF16)
    kept = pltpu.VMEM(rows, BF16)
    sent = pltpu.HBM((devices, 72, DH), F32)
    joined = pltpu.HBM((devices // 2, 72, DH), F32)
    core = lax.axis_index(SEQ[2])[None].astype(jnp.int32)
    scalar = pl.BlockSpec(memory_space=pltpu.SMEM)
    here = pl.BlockSpec(memory_space=pltpu.VMEM)
    there = pl.BlockSpec(memory_space=pl.ANY)
    settings = pltpu.CompilerParams(vmem_limit_bytes=LIMIT)
    queries, key_rows, value_rows, grad_out = map(far, (queries, key_rows, value_rows, grad_out))

    def sems(*n):
        return pltpu.SemaphoreType.DMA(n)

    hp = 4
    local, cum = pl.pallas_call(
        functools.partial(local_kernel, hp),
        in_specs=[here, there, there],
        out_specs=[here] * 2,
        out_shape=[pltpu.VMEM(sent.shape, F32), pltpu.HBM((heads, tokens), F32)],
        scratch_shapes=[kept] * 2 + [sems(heads // hp)] * 2,
        compiler_params=settings,
        name="local_state",
    )(far(log_decay), key_rows, value_rows)
    cum = far(cum)

    mark_shape = pltpu.HBM((8, 128), F32)
    cum_t_shape = pltpu.VMEM((tokens, 128), F32)
    cum_shape = pltpu.VMEM((heads, tokens), F32)
    one_sem = pltpu.SemaphoreType.DMA

    def forward_part(start, count, after, ready):
        hp = 2
        part = pltpu.VMEM((tokens, count * DH), BF16)
        part_t = pltpu.VMEM((count * DH, tokens), BF16)
        *ready, mark = pl.pallas_call(
            functools.partial(forward_kernel, hp, chunks, start),
            in_specs=[there] * (5 + len(ready)),
            out_specs=[there] * 5 + [here],
            out_shape=[flat, pltpu.HBM((width, tokens), BF16), flat, flat, flat, mark_shape],
            scratch_shapes=[part] * 4
            + [part_t]
            + [part] * 3
            + [cum_shape, cum_t_shape, one_sem, sems(3, count // hp), sems(5, count // hp)],
            input_output_aliases={5 + i: i for i in range(len(ready))},
            compiler_params=settings,
            cost_estimate=cost(8e9, 13e6, 3e6),
            name="forward_intra",
        )(cum, queries, key_rows, value_rows, far(after), *map(far, ready))
        return ready, far(mark)

    def backward_part(start, count, after, ready):
        hp = 2
        part = pltpu.VMEM((tokens, count * DH), BF16)
        *ready, mark = pl.pallas_call(
            functools.partial(backward_kernel, hp, chunks, start),
            in_specs=[there] * (7 + len(ready)),
            out_specs=[there] * 3 + [here],
            out_shape=[flat] * 3 + [mark_shape],
            scratch_shapes=[part] * 7
            + [cum_shape, pltpu.VMEM((count, DH, DH), F32), cum_t_shape, one_sem]
            + [sems(count // hp), sems(4, count // hp), sems(3, count // hp)],
            input_output_aliases={7 + i: i for i in range(len(ready))},
            compiler_params=settings,
            cost_estimate=cost(10e9, 15e6, 2e6),
            name="backward_intra",
        )(
            cum, far(state_in), queries, key_rows, value_rows, far(grad_attended), far(after),
            *map(far, ready),
        )
        return ready, far(mark)

    def travel(chip, axes, scan, part, counts):
        got = exchange(chip, axes)
        ready, mark = part(0, counts[0], chip, [])
        passed = scan(got, mark)
        edge = exchange(passed, axes)
        ready, mark = part(counts[0], counts[1], passed, ready)
        edge, last = lax.optimization_barrier((edge, mark))
        return edge, far(last), ready

    sibling = beside(near(local))
    chip = pl.pallas_call(
        combine_forward_kernel,
        in_specs=[scalar, here, here],
        out_specs=here,
        out_shape=joined,
        compiler_params=settings,
        name="combine_forward",
    )(core, near(local), near(sibling))

    def scan_forward(got, mark):
        return pl.pallas_call(
            scan_forward_kernel,
            in_specs=[here, there],
            out_specs=here,
            out_shape=pltpu.HBM((devices // 2, 64, DH), F32),
            compiler_params=settings,
            name="scan_forward",
        )(got, mark)

    chip_state, last, ready = travel(chip, SEQ[:2], scan_forward, forward_part, FORWARD_CUTS)
    sibling_state = beside(chip_state)
    attended_local, turned, grown, faded_k, faded_v = map(far, ready)

    def fetch(after, *arrays):
        return pl.pallas_call(
            fetch_kernel,
            in_specs=[there] * (len(arrays) + 1),
            out_specs=[here] * len(arrays),
            out_shape=[pltpu.VMEM(x.shape, x.dtype) for x in arrays],
            scratch_shapes=[sems(len(arrays))],
            compiler_params=settings,
            cost_estimate=cost(1e9, 19e6),
            name="fetch_rows",
        )(*map(far, arrays), after)

    grown, attended_local, sibling_here = fetch(chip_state, grown, attended_local, sibling)

    hp = 2
    attended, grads, turned, sums, cum_here, state_in = pl.pallas_call(
        functools.partial(sums_kernel, hp),
        in_specs=[scalar] + [here] * 6 + [there] * 4,
        out_specs=[here] * 5 + [there],
        out_shape=[
            pltpu.VMEM(rows, F32),
            kept,
            pltpu.VMEM((width, tokens), BF16),
            pltpu.VMEM((8, tokens), F32),
            pltpu.VMEM((heads, tokens), F32),
            pltpu.HBM((heads, DH, DH), F32),
        ],
        scratch_shapes=[pltpu.VMEM((tokens, 128), F32)] * 2
        + [pltpu.VMEM((heads, DH, DH), F32), sems(heads // hp)]
        + [pltpu.SemaphoreType.DMA] * 3,
        compiler_params=settings,
        name="row_sums",
    )(
        core, chip_state, near(sibling_state), gain, near(grown), near(attended_local),
        near(sibling_here), grad_out, cum, turned, last,
    )

    hp = 4
    others = other_heads(sums)
    sent_grad, output, grad_attended = pl.pallas_call(
        functools.partial(grad_kernel, hp),
        in_specs=[here] * 9,
        out_specs=[here] + [there] * 2,
        out_shape=[pltpu.VMEM(sent.shape, F32), flat, flat],
        scratch_shapes=[pltpu.VMEM((tokens, 128), F32)] * 2 + [kept] * 2 + [sems(2, heads // hp)],
        compiler_params=settings,
        name="grad_state",
    )(near(cum_here), near(turned), near(grads), near(attended), gain, *map(near, (sums, *others)))

    def scan_backward(got_grad, mark):
        return pl.pallas_call(
            scan_backward_kernel,
            in_specs=[here, there],
            out_specs=here,
            out_shape=joined,
            compiler_params=settings,
            name="scan_backward",
        )(got_grad, mark)

    sibling_grad = beside(near(sent_grad))
    chip_grad = pl.pallas_call(
        combine_backward_kernel,
        in_specs=[scalar, here, here],
        out_specs=here,
        out_shape=joined,
        compiler_params=settings,
        name="combine_backward",
    )(core, near(sent_grad), near(sibling_grad))
    chip_after, last_grad, ready = travel(
        chip_grad, SEQ[:2], scan_backward, backward_part, BACKWARD_CUTS
    )
    sibling_after = beside(chip_after)
    grad_q, part_k, part_v = ready

    faded_k, faded_v, sibling_here = fetch(chip_after, faded_k, faded_v, sibling_grad)

    hp = 2
    grad_k, grad_v, grad_gain = pl.pallas_call(
        functools.partial(final_kernel, hp),
        in_specs=[scalar] + [here] * 5 + [there] * 3,
        out_specs=[there] * 2 + [here],
        out_shape=[flat] * 2 + [jax.ShapeDtypeStruct((1, width), F32)],
        scratch_shapes=[kept] * 2 + [sems(2, heads // hp), sems(2, heads // hp)],
        compiler_params=settings,
        name="final_grads",
    )(
        core, chip_after, near(sibling_after), near(faded_k), near(faded_v), near(sibling_here),
        far(part_k), far(part_v), last_grad,
    )
    return output, grad_q, grad_k, grad_v, grad_gain.reshape(width)


def solution(mesh):
    split = Mesh(
        mesh.devices.reshape(4, 4, 2, mesh.shape["head"]), ("seq_0", "seq_1", "seq_2", "head")
    )
    placed = (
        P(SEQ, "head"),
        P(SEQ, "head"),
        P(SEQ, "head"),
        P("head", SEQ),
        P("head"),
        P(SEQ, "head"),
    )
    return jax.shard_map(
        on_device,
        mesh=split,
        in_specs=placed,
        out_specs=(P(SEQ, "head"), P(SEQ, "head"), P(SEQ, "head"), P(SEQ, "head"), P("head")),
        check_vma=False,
    )
```

```python
import functools

import jax
import jax.numpy as jnp
from jax import lax
from jax.experimental import pallas as pl
from jax.experimental.pallas import tpu as pltpu
from jax.sharding import Mesh
from jax.sharding import PartitionSpec as P

DH = 128
HD = 8192
EPSILON = 1e-06
CHUNK = 256
HALF = CHUNK // 2
LIMIT = 28 * 10**6
FORWARD_CUTS = (8, 8)
BACKWARD_CUTS = (8, 8)
SEQ = ("seq_0", "seq_1", "seq_2")
F32 = jnp.float32
BF16 = jnp.bfloat16


def dot(a, b, ca, cb, precision=None):
    return lax.dot_general(
        a, b, (((ca,), (cb,)), ((), ())), precision=precision, preferred_element_type=F32
    )


def lane_prefix(x):
    rows, n = x.shape
    high = x.astype(BF16)
    rest = x - high.astype(F32)
    middle = rest.astype(BF16)
    low = (rest - middle.astype(F32)).astype(BF16)
    blocks = n // 128
    parts = [p[:, 128 * b : 128 * b + 128] for b in range(blocks) for p in (high, middle, low)]
    stacked = jnp.concatenate(parts, axis=0)
    s = lax.broadcasted_iota(jnp.int32, (128, 128), 0)
    t = lax.broadcasted_iota(jnp.int32, (128, 128), 1)
    sums = dot(stacked, (s <= t).astype(BF16), 1, 0)
    out, before = [], jnp.zeros((rows, 1), F32)
    for b in range(blocks):
        first = 3 * rows * b
        inside = (
            sums[first : first + rows]
            + (sums[first + rows : first + 2 * rows] + sums[first + 2 * rows : first + 3 * rows])
        )
        out.append(inside + before)
        before = out[-1][:, 127:]
    return jnp.concatenate(out, axis=1)


def turn(rows_of):
    heads, n = rows_of.shape
    return jnp.concatenate([rows_of, jnp.zeros((128 - heads, n), F32)], axis=0).T


def columns(cum_t_ref, first):
    return pltpu.roll(cum_t_ref[...], lax.rem(128 - first, 128), 1)


def pair(first, second):
    zero = jnp.zeros_like(first)
    return jnp.concatenate(
        [jnp.concatenate([first, zero], axis=1), jnp.concatenate([zero, second], axis=1)], axis=0
    )


def lanes_of(h, n=1):
    return pl.ds(pl.multiple_of(h * DH, DH), n * DH)


def over_heads(count, step, body):
    lax.fori_loop(0, count // step, lambda i, c: (body(i, i * step), c)[1], 0)


def begin(arrive, steps, ahead):
    for i in range(min(ahead, steps)):
        for copy in arrive(i):
            copy.start()


def next_piece(arrive, step, steps, ahead):
    for copy in arrive(step):
        copy.wait()

    @pl.when(step + ahead < steps)
    def _():
        for copy in arrive(step + ahead):
            copy.start()


def copy_piece(source, target, sems, i, n):
    at = lanes_of(i * n, n)
    return pltpu.make_async_copy(source.at[:, at], target.at[:, at], sems.at[i])


def send_state(state_ref, h, s, extra):
    for half in range(2):
        state_ref[2 * h + half, 0:64] = s[64 * half : 64 * half + 64]
        state_ref[2 * h + half, 64:72] = jnp.broadcast_to(extra, (8, 128))


def local_kernel(hp, ld_ref, k_in, v_in, state_ref, cum_ref, k_ref, v_ref, k_sem, v_sem):
    heads = ld_ref.shape[0]

    def arrive(i):
        return copy_piece(k_in, k_ref, k_sem, i, hp), copy_piece(v_in, v_ref, v_sem, i, hp)

    begin(arrive, heads // hp, 3)
    cum_ref[...] = lane_prefix(ld_ref[...])

    def body(i, first):
        next_piece(arrive, i, heads // hp, 3)
        for j in range(hp):
            at = lanes_of(first + j)
            row = cum_ref[pl.ds(first + j, 1), :]
            end = row[:, -1:]
            k = late(k_ref[:, at], row, end)
            send_state(state_ref, first + j, dot(k, v_ref[:, at], 1, 0), jnp.exp(end))

    over_heads(heads, hp, body)


def late(k, row, end):
    return (k.T.astype(F32) * jnp.exp(end - row)).astype(BF16)


def triangle(row, col):
    s = lax.broadcasted_iota(jnp.int32, (HALF, HALF), 0)
    t = lax.broadcasted_iota(jnp.int32, (HALF, HALF), 1)
    return jnp.where(s <= t, jnp.exp(row - col), 0.0)


def attend(q, k, v, col, row):
    t = lax.broadcasted_iota(jnp.int32, (CHUNK, CHUNK), 0)
    s = lax.broadcasted_iota(jnp.int32, (CHUNK, CHUNK), 1)
    decay = jnp.where(t >= s, jnp.exp(col - row), 0.0)
    return dot((dot(q, k, 1, 1) * decay).astype(BF16), v, 1, 0)


def attend_back(q, k, v, ga, col, row):
    decay = jnp.concatenate(
        [triangle(row[:, :HALF], col[:HALF]), jnp.exp(row[:, HALF:] - col[:HALF])], axis=1
    )
    w0 = (dot(k[:HALF], q, 1, 1) * decay).astype(BF16)
    g0 = (dot(v[:HALF], ga, 1, 1) * decay).astype(BF16)
    decay = triangle(row[:, HALF:], col[HALF:])
    w1 = (dot(k[HALF:], q[HALF:], 1, 1) * decay).astype(BF16)
    g1 = (dot(v[HALF:], ga[HALF:], 1, 1) * decay).astype(BF16)
    gk = jnp.concatenate([dot(g0, q, 1, 0), dot(g1, q[HALF:], 1, 0)], axis=0)
    gv = jnp.concatenate([dot(w0, ga, 1, 0), dot(w1, ga[HALF:], 1, 0)], axis=0)
    late_g = jnp.concatenate([g0[:, HALF:], g1], axis=0)
    gq = jnp.concatenate([dot(g0[:, :HALF], k[:HALF], 0, 0), dot(late_g, k, 0, 0)], axis=0)
    return gq, gk, gv


def forward_kernel(hp, n, start, cum_in, q_in, k_in, v_in, after_ref, *refs):
    out_hbm, turned_hbm, qd_hbm, kd_hbm, vd_hbm, mark_ref = refs[-19:-13]
    q_ref, k_ref, v_ref, out_ref, turned_ref, qd_ref, kd_ref, vd_ref = refs[-13:-5]
    cum_ref, cum_t_ref, cum_sem, in_sem, out_sem = refs[-5:]
    cum_copy = pltpu.make_async_copy(cum_in, cum_ref, cum_sem)
    cum_copy.start()
    mark_ref[...] = jnp.zeros_like(mark_ref)
    count = out_ref.shape[1] // DH
    into = ((q_in, q_ref), (k_in, k_ref), (v_in, v_ref))
    out = ((out_ref, out_hbm), (qd_ref, qd_hbm), (kd_ref, kd_hbm), (vd_ref, vd_hbm))

    def spots(step):
        return lanes_of(step * hp, hp), lanes_of(start + step * hp, hp)

    def arrive(step):
        near_at, far_at = spots(step)
        return [
            pltpu.make_async_copy(a.at[:, far_at], b.at[:, near_at], in_sem.at[j, step])
            for j, (a, b) in enumerate(into)
        ]

    def leave(step):
        near_at, far_at = spots(step)
        return [
            pltpu.make_async_copy(a.at[:, near_at], b.at[:, far_at], out_sem.at[j, step])
            for j, (a, b) in enumerate(out)
        ] + [
            pltpu.make_async_copy(
                turned_ref.at[near_at], turned_hbm.at[far_at], out_sem.at[len(out), step]
            )
        ]

    begin(arrive, count // hp, 1)
    cum_copy.wait()
    cum_t_ref[...] = turn(cum_ref[...])

    def body(step, first):
        next_piece(arrive, step, count // hp, 1)
        cols = columns(cum_t_ref, start + first)
        growth = jnp.exp(cols)
        tail = jnp.exp(cols[-1:, :] - cols)
        for i in range(hp):
            lanes = lanes_of(first + i)
            qd = (q_ref[:, lanes].astype(F32) * growth[:, i : i + 1]).astype(BF16)
            qd_ref[:, lanes] = qd
            turned_ref[lanes, :] = qd.T
            tail_i = jnp.broadcast_to(tail[:, i : i + 1], (tail.shape[0], DH))
            kd_ref[:, lanes] = (k_ref[:, lanes].astype(F32) * tail_i).astype(BF16)
            vd_ref[:, lanes] = (v_ref[:, lanes].astype(F32) * tail_i).astype(BF16)
            state = None
            base = jnp.zeros((1, 1), F32)
            for j in range(n):
                at = slice(j * CHUNK, (j + 1) * CHUNK)
                col = cols[at, i : i + 1]
                end = col[CHUNK - 1 :, :]
                row = cum_ref[pl.ds(start + first + i, 1), at]
                q, k, v = q_ref[at, lanes], k_ref[at, lanes], v_ref[at, lanes]
                a = attend(q, k, v, col, row)
                if j > 0:
                    a = a + jnp.exp(col - base) * dot(q, state.astype(BF16), 1, 0)
                out_ref[at, lanes] = a.astype(BF16)
                if j < n - 1:
                    new = dot(late(k, row, end), v, 1, 0)
                    state = new if state is None else state * jnp.exp(end - base) + new
                base = end
        for copy in leave(step):
            copy.start()

    over_heads(count, hp, body)
    for step in range(count // hp):
        for copy in leave(step):
            copy.wait()


def fetch_kernel(*refs):
    n = (len(refs) - 2) // 2
    sems = refs[-1]
    copies = [pltpu.make_async_copy(refs[i], refs[n + 1 + i], sems.at[i]) for i in range(n)]
    for copy in copies:
        copy.start()
    for copy in copies:
        copy.wait()


def sums_kernel(
    hp, core_ref, mine_ref, theirs_ref, gain_ref, q_ref, a_ref, sibling_ref, g_in, cum_in, turned_in,
    after_ref, att_ref, g_ref, turned_ref, sum_ref, cum_ref, s_hbm,
    sq, cross, s_ref, g_sem, turned_sem, s_sem, cum_sem,
):
    heads = s_ref.shape[0]
    for i in range(heads // hp):
        copy_piece(g_in, g_ref, g_sem, i, hp).start()
    core = core_ref[0]

    def assemble(h, carry):
        for half in range(2):
            s_ref[h, 64 * half : 64 * half + 64] = half_state(
                core, 2 * h + half, mine_ref, theirs_ref, sibling_ref, 1, 64
            )
        return carry

    cum_copy = pltpu.make_async_copy(cum_in, cum_ref, cum_sem)
    cum_copy.start()
    turned = pltpu.make_async_copy(turned_in, turned_ref, turned_sem)
    turned.start()
    lax.fori_loop(0, heads, assemble, 0)
    leave = pltpu.make_async_copy(s_ref, s_hbm, s_sem)
    leave.start()
    sq[...] = jnp.zeros_like(sq)
    cross[...] = jnp.zeros_like(cross)

    def body(step, first):
        copy_piece(g_in, g_ref, g_sem, step, hp).wait()
        sq_sum, cross_sum = sq[...], cross[...]
        for i in range(0, hp, 2):
            h = first + i
            lanes = lanes_of(h, 2)
            both = pair(s_ref[h].astype(BF16), s_ref[h + 1].astype(BF16))
            att = a_ref[:, lanes].astype(F32) + dot(q_ref[:, lanes], both, 1, 0)
            att_ref[:, lanes] = att
            gg = g_ref[:, lanes].astype(F32) * gain_ref[:, lanes]
            square, product = att * att, gg * att
            sq_sum = sq_sum + (square[:, :DH] + square[:, DH:])
            cross_sum = cross_sum + (product[:, :DH] + product[:, DH:])
        sq[...] = sq_sum
        cross[...] = cross_sum

    over_heads(heads, hp, body)
    a = jnp.sum(sq[...].T, axis=0, keepdims=True)
    b = jnp.sum(cross[...].T, axis=0, keepdims=True)
    which = lax.broadcasted_iota(jnp.int32, sum_ref.shape, 0)
    sum_ref[...] = jnp.where(which == 0, a, b)
    turned.wait()
    cum_copy.wait()
    leave.wait()


def grad_kernel(
    hp, cum_ref, turned_ref, g_ref, att_ref, gain_ref, s0, s1, s2, s3, state_ref, out_hbm, ga_hbm,
    inv_ref, both_ref, out_ref, ga_ref, out_sem,
):
    sums = (s0[...] + s1[...]) + (s2[...] + s3[...])
    inverse = lax.rsqrt(sums[0:1] / HD + EPSILON)
    center = sums[1:2] * inverse / HD
    both = inverse * inverse * center
    length = both.shape[1]
    inv_ref[...] = jnp.broadcast_to(inverse, (128, length)).T
    both_ref[...] = jnp.broadcast_to(both, (128, length)).T
    heads = state_ref.shape[0] // 2
    which = lax.broadcasted_iota(jnp.int32, (8, DH), 0)

    def leave(step):
        return (
            copy_piece(out_ref, out_hbm, out_sem.at[0], step, hp),
            copy_piece(ga_ref, ga_hbm, out_sem.at[1], step, hp),
        )

    def body(step, first):
        inverse, both = inv_ref[...], both_ref[...]
        for i in range(hp):
            lanes = lanes_of(first + i)
            att = att_ref[:, lanes]
            gain = gain_ref[:, lanes]
            scaled = g_ref[:, lanes].astype(F32) * inverse
            ga = (scaled * gain - both * att).astype(BF16)
            ga_ref[:, lanes] = ga
            out_ref[:, lanes] = (att * inverse * gain).astype(BF16)
            gain_part = jnp.sum(scaled * att, axis=0, keepdims=True)
            turned = turned_ref[pl.ds(pl.multiple_of((first + i) * DH, DH), DH), :]
            decay = jnp.exp(cum_ref[pl.ds(first + i, 1), :][:, -1:])
            extra = jnp.where(which == 0, gain_part, decay)
            send_state(state_ref, first + i, dot(turned, ga, 1, 0), extra)
        for copy in leave(step):
            copy.start()

    over_heads(heads, hp, body)
    for step in range(heads // hp):
        for copy in leave(step):
            copy.wait()


def backward_kernel(
    hp, n, start, cum_in, s_in, q_in, k_in, v_in, ga_in, after_ref, *refs
):
    gq_hbm, gk_hbm, gv_hbm, mark_ref = refs[-18:-14]
    q_ref, k_ref, v_ref, ga_ref, gq_ref, gk_ref, gv_ref = refs[-14:-7]
    cum_ref, s_ref, cum_t_ref, cum_sem, s_sem, in_sem, out_sem = refs[-7:]
    cum_copy = pltpu.make_async_copy(cum_in, cum_ref, cum_sem)
    cum_copy.start()
    mark_ref[...] = jnp.zeros_like(mark_ref)
    count = gk_ref.shape[1] // DH
    into = ((q_in, q_ref), (k_in, k_ref), (v_in, v_ref), (ga_in, ga_ref))
    out = ((gq_ref, gq_hbm), (gk_ref, gk_hbm), (gv_ref, gv_hbm))

    def spots(step):
        return lanes_of(step * hp, hp), lanes_of(start + step * hp, hp)

    def arrive(step):
        near_at, far_at = spots(step)
        return [
            pltpu.make_async_copy(a.at[:, far_at], b.at[:, near_at], in_sem.at[j, step])
            for j, (a, b) in enumerate(into)
        ] + [
            pltpu.make_async_copy(
                s_in.at[pl.ds(start + step * hp, hp)], s_ref.at[pl.ds(step * hp, hp)], s_sem.at[step]
            )
        ]

    def leave(step):
        near_at, far_at = spots(step)
        return [
            pltpu.make_async_copy(a.at[:, near_at], b.at[:, far_at], out_sem.at[j, step])
            for j, (a, b) in enumerate(out)
        ]

    begin(arrive, count // hp, 1)
    cum_copy.wait()
    cum_t_ref[...] = turn(cum_ref[...])

    def body(step, first):
        next_piece(arrive, step, count // hp, 1)
        cols = columns(cum_t_ref, start + first)
        for i in range(hp):
            h = start + first + i
            lanes = lanes_of(first + i)
            states = [s_ref[first + i]]
            ends = [jnp.zeros((1, 1), F32)]
            for j in range(n):
                at = slice(j * CHUNK, (j + 1) * CHUNK)
                col = cols[at, i : i + 1]
                end = col[CHUNK - 1 :, :]
                if j < n - 1:
                    row = cum_ref[pl.ds(h, 1), at]
                    kd = late(k_ref[at, lanes], row, end)
                    states.append(
                        states[-1] * jnp.exp(end - ends[-1]) + dot(kd, v_ref[at, lanes], 1, 0)
                    )
                ends.append(end)
            after = None
            for j in reversed(range(n)):
                at = slice(j * CHUNK, (j + 1) * CHUNK)
                col = cols[at, i : i + 1]
                row = cum_ref[pl.ds(h, 1), at]
                q, k, v = q_ref[at, lanes], k_ref[at, lanes], v_ref[at, lanes]
                ga = ga_ref[at, lanes]
                gq, gk, gv = attend_back(q, k, v, ga, col, row)
                gq = gq + jnp.exp(col - ends[j]) * dot(ga, states[j].astype(BF16), 1, 1)
                if after is not None:
                    tail = jnp.exp(ends[j + 1] - col)
                    low = after.astype(BF16)
                    gk = gk + tail * dot(v, low, 1, 1)
                    gv = gv + tail * dot(k, low, 1, 0)
                gq_ref[at, lanes] = gq.astype(BF16)
                gk_ref[at, lanes] = gk.astype(BF16)
                gv_ref[at, lanes] = gv.astype(BF16)
                if j > 0:
                    qd = (q.T.astype(F32) * jnp.exp(row - ends[j])).astype(BF16)
                    new = dot(qd, ga, 1, 0)
                    after = new if after is None else after * jnp.exp(ends[j + 1] - ends[j]) + new
        for copy in leave(step):
            copy.start()

    over_heads(count, hp, body)
    for step in range(count // hp):
        for copy in leave(step):
            copy.wait()


def final_kernel(
    hp, core_ref, mine_ref, theirs_ref, k_ref, v_ref, sibling_ref, gk_in, gv_in, after_ref,
    gk_hbm, gv_hbm, gain_ref, gk_ref, gv_ref, in_sem, out_sem,
):
    core = core_ref[0]
    into = ((gk_in, gk_ref), (gv_in, gv_ref))
    heads = sibling_ref.shape[0] // 2

    def arrive(step):
        return [copy_piece(a, b, in_sem.at[j], step, hp) for j, (a, b) in enumerate(into)]

    def leave(step):
        return (
            copy_piece(gk_ref, gk_hbm, out_sem.at[0], step, hp),
            copy_piece(gv_ref, gv_hbm, out_sem.at[1], step, hp),
        )

    for i in range(heads // hp):
        for copy in arrive(i):
            copy.start()

    def body(step, first):
        for copy in arrive(step):
            copy.wait()
        for i in range(0, hp, 2):
            h = first + i
            lanes = lanes_of(h, 2)
            states = []
            for j in (h, h + 1):
                halves = [
                    half_state(core, m, mine_ref, theirs_ref, sibling_ref, 0, 65)
                    for m in (2 * j, 2 * j + 1)
                ]
                n = mine_ref.shape[0]
                own = (2 * j >= core * n) & (2 * j < core * n + n)
                at = lax.rem(2 * j, n)
                gain_ref[:, lanes_of(j)] = jnp.where(
                    own, mine_ref[at, 64:65], theirs_ref[at, 64:65]
                )
                states.append(jnp.concatenate(halves, axis=0).astype(BF16))
            both = pair(*states)
            gk_ref[:, lanes] = (
                gk_ref[:, lanes].astype(F32) + dot(v_ref[:, lanes], both, 1, 1)
            ).astype(BF16)
            gv_ref[:, lanes] = (
                gv_ref[:, lanes].astype(F32) + dot(k_ref[:, lanes], both, 1, 0)
            ).astype(BF16)
        for copy in leave(step):
            copy.start()

    over_heads(heads, hp, body)
    for step in range(heads // hp):
        for copy in leave(step):
            copy.wait()


def by_core(core, mine, theirs):
    return jnp.where(core == 0, mine, theirs), jnp.where(core == 0, theirs, mine)


def combine_forward_kernel(core_ref, mine_ref, theirs_ref, out_ref):
    core = core_ref[0]
    n = out_ref.shape[0]
    for i in range(n):
        at = core * n + i
        first, second = by_core(core, mine_ref[at], theirs_ref[at])
        decay = second[64:65]
        out_ref[i, 0:64] = first[0:64] * decay + second[0:64]
        out_ref[i, 64:72] = first[64:72] * second[64:72]


def combine_backward_kernel(core_ref, mine_ref, theirs_ref, out_ref):
    core = core_ref[0]
    n = out_ref.shape[0]
    which = lax.broadcasted_iota(jnp.int32, (8, DH), 0)
    for i in range(n):
        at = core * n + i
        first, second = by_core(core, mine_ref[at], theirs_ref[at])
        out_ref[i, 0:64] = second[0:64] * first[65:66] + first[0:64]
        out_ref[i, 64:72] = jnp.where(
            which == 0, first[64:72] + second[64:72], first[64:72] * second[64:72]
        )


def scan_forward_kernel(x_ref, mark_ref, out_ref):
    n = x_ref.shape[0]
    state = jnp.zeros((64, 128), F32)
    for j in range(n):
        out_ref[j] = state
        if j < n - 1:
            state = state * x_ref[j, 64:65] + x_ref[j, 0:64]


def scan_backward_kernel(x_ref, mark_ref, out_ref):
    n = x_ref.shape[0]
    state = jnp.zeros((64, 128), F32)
    gain = jnp.zeros((8, 128), F32)
    for j in reversed(range(n)):
        out_ref[j, 0:64] = state
        state = state * x_ref[j, 65:66] + x_ref[j, 0:64]
        gain = gain + x_ref[j, 64:72]
    for j in range(n):
        out_ref[j, 64:72] = gain


def half_state(core, m, mine_ref, theirs_ref, sibling_ref, last, row):
    n = mine_ref.shape[0]
    here = core * n
    own = (m >= here) & (m < here + n)
    at = lax.rem(m, n)
    value = jnp.where(own, mine_ref[at, 0:64], theirs_ref[at, 0:64])
    beside = sibling_ref[m]
    return jnp.where(core == last, value * beside[row : row + 1] + beside[0:64], value)


def cost(flops, moved, exps=0):
    return pl.CostEstimate(flops=int(flops), bytes_accessed=int(moved), transcendentals=int(exps))


def far(x):
    return pltpu.with_memory_space_constraint(x, pltpu.HBM)


def near(x):
    return pltpu.with_memory_space_constraint(x, pltpu.VMEM)


def exchange(x, axes):
    return lax.all_to_all(x, axes, split_axis=0, concat_axis=0, tiled=True)


def beside(x):
    return lax.ppermute(x, SEQ[2], [(0, 1), (1, 0)])


def other_heads(sums):
    groups = lax.axis_size("head")
    return [
        lax.ppermute(sums, "head", [(i, (i + shift) % groups) for i in range(groups)])
        for shift in range(1, groups)
    ]


def on_device(queries, key_rows, value_rows, log_decay, norm_gain, grad_out):
    tokens, width = queries.shape
    heads = width // DH
    devices = 2 * heads
    chunks = tokens // CHUNK
    gain = norm_gain[None, :]
    rows = (tokens, width)
    flat = pltpu.HBM(rows, BF16)
    kept = pltpu.VMEM(rows, BF16)
    sent = pltpu.HBM((devices, 72, DH), F32)
    joined = pltpu.HBM((devices // 2, 72, DH), F32)
    core = lax.axis_index(SEQ[2])[None].astype(jnp.int32)
    scalar = pl.BlockSpec(memory_space=pltpu.SMEM)
    here = pl.BlockSpec(memory_space=pltpu.VMEM)
    there = pl.BlockSpec(memory_space=pl.ANY)
    settings = pltpu.CompilerParams(vmem_limit_bytes=LIMIT)
    queries, key_rows, value_rows, grad_out = map(far, (queries, key_rows, value_rows, grad_out))

    def sems(*n):
        return pltpu.SemaphoreType.DMA(n)

    hp = 4
    local, cum = pl.pallas_call(
        functools.partial(local_kernel, hp),
        in_specs=[here, there, there],
        out_specs=[here] * 2,
        out_shape=[pltpu.VMEM(sent.shape, F32), pltpu.HBM((heads, tokens), F32)],
        scratch_shapes=[kept] * 2 + [sems(heads // hp)] * 2,
        compiler_params=settings,
        name="local_state",
    )(far(log_decay), key_rows, value_rows)
    cum = far(cum)

    mark_shape = pltpu.HBM((8, 128), F32)
    cum_t_shape = pltpu.VMEM((tokens, 128), F32)
    cum_shape = pltpu.VMEM((heads, tokens), F32)
    one_sem = pltpu.SemaphoreType.DMA

    def forward_part(start, count, after, ready):
        hp = 2
        part = pltpu.VMEM((tokens, count * DH), BF16)
        part_t = pltpu.VMEM((count * DH, tokens), BF16)
        *ready, mark = pl.pallas_call(
            functools.partial(forward_kernel, hp, chunks, start),
            in_specs=[there] * (5 + len(ready)),
            out_specs=[there] * 5 + [here],
            out_shape=[flat, pltpu.HBM((width, tokens), BF16), flat, flat, flat, mark_shape],
            scratch_shapes=[part] * 4
            + [part_t]
            + [part] * 3
            + [cum_shape, cum_t_shape, one_sem, sems(3, count // hp), sems(5, count // hp)],
            input_output_aliases={5 + i: i for i in range(len(ready))},
            compiler_params=settings,
            cost_estimate=cost(8e9, 13e6, 3e6),
            name="forward_intra",
        )(cum, queries, key_rows, value_rows, far(after), *map(far, ready))
        return ready, far(mark)

    def backward_part(start, count, after, ready):
        hp = 2
        part = pltpu.VMEM((tokens, count * DH), BF16)
        *ready, mark = pl.pallas_call(
            functools.partial(backward_kernel, hp, chunks, start),
            in_specs=[there] * (7 + len(ready)),
            out_specs=[there] * 3 + [here],
            out_shape=[flat] * 3 + [mark_shape],
            scratch_shapes=[part] * 7
            + [cum_shape, pltpu.VMEM((count, DH, DH), F32), cum_t_shape, one_sem]
            + [sems(count // hp), sems(4, count // hp), sems(3, count // hp)],
            input_output_aliases={7 + i: i for i in range(len(ready))},
            compiler_params=settings,
            cost_estimate=cost(10e9, 15e6, 2e6),
            name="backward_intra",
        )(
            cum, far(state_in), queries, key_rows, value_rows, far(grad_attended), far(after),
            *map(far, ready),
        )
        return ready, far(mark)

    def travel(chip, axes, scan, part, counts):
        got = exchange(chip, axes)
        ready, mark = part(0, counts[0], chip, [])
        passed = scan(got, mark)
        edge = exchange(passed, axes)
        ready, mark = part(counts[0], counts[1], passed, ready)
        edge, last = lax.optimization_barrier((edge, mark))
        return edge, far(last), ready

    sibling = beside(near(local))
    chip = pl.pallas_call(
        combine_forward_kernel,
        in_specs=[scalar, here, here],
        out_specs=here,
        out_shape=joined,
        compiler_params=settings,
        name="combine_forward",
    )(core, near(local), near(sibling))

    def scan_forward(got, mark):
        return pl.pallas_call(
            scan_forward_kernel,
            in_specs=[here, there],
            out_specs=here,
            out_shape=pltpu.HBM((devices // 2, 64, DH), F32),
            compiler_params=settings,
            name="scan_forward",
        )(got, mark)

    chip_state, last, ready = travel(chip, SEQ[:2], scan_forward, forward_part, FORWARD_CUTS)
    sibling_state = beside(chip_state)
    attended_local, turned, grown, faded_k, faded_v = map(far, ready)

    def fetch(after, *arrays):
        return pl.pallas_call(
            fetch_kernel,
            in_specs=[there] * (len(arrays) + 1),
            out_specs=[here] * len(arrays),
            out_shape=[pltpu.VMEM(x.shape, x.dtype) for x in arrays],
            scratch_shapes=[sems(len(arrays))],
            compiler_params=settings,
            cost_estimate=cost(1e9, 19e6),
            name="fetch_rows",
        )(*map(far, arrays), after)

    grown, attended_local, sibling_here = fetch(chip_state, grown, attended_local, sibling)

    hp = 2
    attended, grads, turned, sums, cum_here, state_in = pl.pallas_call(
        functools.partial(sums_kernel, hp),
        in_specs=[scalar] + [here] * 6 + [there] * 4,
        out_specs=[here] * 5 + [there],
        out_shape=[
            pltpu.VMEM(rows, F32),
            kept,
            pltpu.VMEM((width, tokens), BF16),
            pltpu.VMEM((8, tokens), F32),
            pltpu.VMEM((heads, tokens), F32),
            pltpu.HBM((heads, DH, DH), F32),
        ],
        scratch_shapes=[pltpu.VMEM((tokens, 128), F32)] * 2
        + [pltpu.VMEM((heads, DH, DH), F32), sems(heads // hp)]
        + [pltpu.SemaphoreType.DMA] * 3,
        compiler_params=settings,
        name="row_sums",
    )(
        core, chip_state, near(sibling_state), gain, near(grown), near(attended_local),
        near(sibling_here), grad_out, cum, turned, last,
    )

    hp = 4
    others = other_heads(sums)
    sent_grad, output, grad_attended = pl.pallas_call(
        functools.partial(grad_kernel, hp),
        in_specs=[here] * 9,
        out_specs=[here] + [there] * 2,
        out_shape=[pltpu.VMEM(sent.shape, F32), flat, flat],
        scratch_shapes=[pltpu.VMEM((tokens, 128), F32)] * 2 + [kept] * 2 + [sems(2, heads // hp)],
        compiler_params=settings,
        name="grad_state",
    )(near(cum_here), near(turned), near(grads), near(attended), gain, *map(near, (sums, *others)))

    def scan_backward(got_grad, mark):
        return pl.pallas_call(
            scan_backward_kernel,
            in_specs=[here, there],
            out_specs=here,
            out_shape=joined,
            compiler_params=settings,
            name="scan_backward",
        )(got_grad, mark)

    sibling_grad = beside(near(sent_grad))
    chip_grad = pl.pallas_call(
        combine_backward_kernel,
        in_specs=[scalar, here, here],
        out_specs=here,
        out_shape=joined,
        compiler_params=settings,
        name="combine_backward",
    )(core, near(sent_grad), near(sibling_grad))
    chip_after, last_grad, ready = travel(
        chip_grad, SEQ[:2], scan_backward, backward_part, BACKWARD_CUTS
    )
    sibling_after = beside(chip_after)
    grad_q, part_k, part_v = ready

    faded_k, faded_v, sibling_here = fetch(chip_after, faded_k, faded_v, sibling_grad)

    hp = 2
    grad_k, grad_v, grad_gain = pl.pallas_call(
        functools.partial(final_kernel, hp),
        in_specs=[scalar] + [here] * 5 + [there] * 3,
        out_specs=[there] * 2 + [here],
        out_shape=[flat] * 2 + [jax.ShapeDtypeStruct((1, width), F32)],
        scratch_shapes=[kept] * 2 + [sems(2, heads // hp), sems(2, heads // hp)],
        compiler_params=settings,
        name="final_grads",
    )(
        core, chip_after, near(sibling_after), near(faded_k), near(faded_v), near(sibling_here),
        far(part_k), far(part_v), last_grad,
    )
    return output, grad_q, grad_k, grad_v, grad_gain.reshape(width)


def solution(mesh):
    split = Mesh(
        mesh.devices.reshape(4, 4, 2, mesh.shape["head"]), ("seq_0", "seq_1", "seq_2", "head")
    )
    placed = (
        P(SEQ, "head"),
        P(SEQ, "head"),
        P(SEQ, "head"),
        P("head", SEQ),
        P("head"),
        P(SEQ, "head"),
    )
    return jax.shard_map(
        on_device,
        mesh=split,
        in_specs=placed,
        out_specs=(P(SEQ, "head"), P(SEQ, "head"), P(SEQ, "head"), P(SEQ, "head"), P("head")),
        check_vma=False,
    )
```

```python
import functools

import jax
import jax.numpy as jnp
from jax import lax
from jax.experimental import pallas as pl
from jax.experimental.pallas import tpu as pltpu
from jax.sharding import Mesh
from jax.sharding import PartitionSpec as P

DH = 128
HD = 8192
EPSILON = 1e-06
CHUNK = 256
HALF = CHUNK // 2
LIMIT = 28 * 10**6
FORWARD_CUTS = (8, 8)
BACKWARD_CUTS = (8, 8)
SEQ = ("seq_0", "seq_1", "seq_2")
F32 = jnp.float32
BF16 = jnp.bfloat16


def dot(a, b, ca, cb, precision=None):
    return lax.dot_general(
        a, b, (((ca,), (cb,)), ((), ())), precision=precision, preferred_element_type=F32
    )


def lane_prefix(x):
    rows, n = x.shape
    high = x.astype(BF16)
    rest = x - high.astype(F32)
    middle = rest.astype(BF16)
    low = (rest - middle.astype(F32)).astype(BF16)
    blocks = n // 128
    parts = [p[:, 128 * b : 128 * b + 128] for b in range(blocks) for p in (high, middle, low)]
    stacked = jnp.concatenate(parts, axis=0)
    s = lax.broadcasted_iota(jnp.int32, (128, 128), 0)
    t = lax.broadcasted_iota(jnp.int32, (128, 128), 1)
    sums = dot(stacked, (s <= t).astype(BF16), 1, 0)
    out, before = [], jnp.zeros((rows, 1), F32)
    for b in range(blocks):
        first = 3 * rows * b
        inside = (
            sums[first : first + rows]
            + (sums[first + rows : first + 2 * rows] + sums[first + 2 * rows : first + 3 * rows])
        )
        out.append(inside + before)
        before = out[-1][:, 127:]
    return jnp.concatenate(out, axis=1)


def turn(rows_of):
    heads, n = rows_of.shape
    return jnp.concatenate([rows_of, jnp.zeros((128 - heads, n), F32)], axis=0).T


def columns(cum_t_ref, first):
    return pltpu.roll(cum_t_ref[...], lax.rem(128 - first, 128), 1)


def pair(first, second):
    zero = jnp.zeros_like(first)
    return jnp.concatenate(
        [jnp.concatenate([first, zero], axis=1), jnp.concatenate([zero, second], axis=1)], axis=0
    )


def lanes_of(h, n=1):
    return pl.ds(pl.multiple_of(h * DH, DH), n * DH)


def over_heads(count, step, body):
    lax.fori_loop(0, count // step, lambda i, c: (body(i, i * step), c)[1], 0)


def begin(arrive, steps, ahead):
    for i in range(min(ahead, steps)):
        for copy in arrive(i):
            copy.start()


def next_piece(arrive, step, steps, ahead):
    for copy in arrive(step):
        copy.wait()

    @pl.when(step + ahead < steps)
    def _():
        for copy in arrive(step + ahead):
            copy.start()


def copy_piece(source, target, sems, i, n):
    at = lanes_of(i * n, n)
    return pltpu.make_async_copy(source.at[:, at], target.at[:, at], sems.at[i])


def send_state(state_ref, h, s, extra):
    for half in range(2):
        state_ref[2 * h + half, 0:64] = s[64 * half : 64 * half + 64]
        state_ref[2 * h + half, 64:72] = jnp.broadcast_to(extra, (8, 128))


def local_kernel(hp, ld_ref, k_in, v_in, state_ref, cum_ref, k_ref, v_ref, k_sem, v_sem):
    heads = ld_ref.shape[0]

    def arrive(i):
        return copy_piece(k_in, k_ref, k_sem, i, hp), copy_piece(v_in, v_ref, v_sem, i, hp)

    begin(arrive, heads // hp, 3)
    cum_ref[...] = lane_prefix(ld_ref[...])

    def body(i, first):
        next_piece(arrive, i, heads // hp, 3)
        for j in range(hp):
            at = lanes_of(first + j)
            row = cum_ref[pl.ds(first + j, 1), :]
            end = row[:, -1:]
            k = late(k_ref[:, at], row, end)
            send_state(state_ref, first + j, dot(k, v_ref[:, at], 1, 0), jnp.exp(end))

    over_heads(heads, hp, body)


def late(k, row, end):
    return (k.T.astype(F32) * jnp.exp(end - row)).astype(BF16)


def triangle(row, col):
    s = lax.broadcasted_iota(jnp.int32, (HALF, HALF), 0)
    t = lax.broadcasted_iota(jnp.int32, (HALF, HALF), 1)
    return jnp.where(s <= t, jnp.exp(row - col), 0.0)


def attend(q, k, v, col, row):
    t = lax.broadcasted_iota(jnp.int32, (CHUNK, CHUNK), 0)
    s = lax.broadcasted_iota(jnp.int32, (CHUNK, CHUNK), 1)
    decay = jnp.where(t >= s, jnp.exp(col - row), 0.0)
    return dot((dot(q, k, 1, 1) * decay).astype(BF16), v, 1, 0)


def attend_back(q, k, v, ga, col, row):
    decay = jnp.concatenate(
        [triangle(row[:, :HALF], col[:HALF]), jnp.exp(row[:, HALF:] - col[:HALF])], axis=1
    )
    w0 = (dot(k[:HALF], q, 1, 1) * decay).astype(BF16)
    g0 = (dot(v[:HALF], ga, 1, 1) * decay).astype(BF16)
    decay = triangle(row[:, HALF:], col[HALF:])
    w1 = (dot(k[HALF:], q[HALF:], 1, 1) * decay).astype(BF16)
    g1 = (dot(v[HALF:], ga[HALF:], 1, 1) * decay).astype(BF16)
    gk = jnp.concatenate([dot(g0, q, 1, 0), dot(g1, q[HALF:], 1, 0)], axis=0)
    gv = jnp.concatenate([dot(w0, ga, 1, 0), dot(w1, ga[HALF:], 1, 0)], axis=0)
    late_g = jnp.concatenate([g0[:, HALF:], g1], axis=0)
    gq = jnp.concatenate([dot(g0[:, :HALF], k[:HALF], 0, 0), dot(late_g, k, 0, 0)], axis=0)
    return gq, gk, gv


def forward_kernel(hp, n, start, cum_in, q_in, k_in, v_in, after_ref, *refs):
    out_hbm, turned_hbm, qd_hbm, kd_hbm, vd_hbm, mark_ref = refs[-19:-13]
    q_ref, k_ref, v_ref, out_ref, turned_ref, qd_ref, kd_ref, vd_ref = refs[-13:-5]
    cum_ref, cum_t_ref, cum_sem, in_sem, out_sem = refs[-5:]
    cum_copy = pltpu.make_async_copy(cum_in, cum_ref, cum_sem)
    cum_copy.start()
    mark_ref[...] = jnp.zeros_like(mark_ref)
    count = out_ref.shape[1] // DH
    into = ((q_in, q_ref), (k_in, k_ref), (v_in, v_ref))
    out = ((out_ref, out_hbm), (qd_ref, qd_hbm), (kd_ref, kd_hbm), (vd_ref, vd_hbm))

    def spots(step):
        return lanes_of(step * hp, hp), lanes_of(start + step * hp, hp)

    def arrive(step):
        near_at, far_at = spots(step)
        return [
            pltpu.make_async_copy(a.at[:, far_at], b.at[:, near_at], in_sem.at[j, step])
            for j, (a, b) in enumerate(into)
        ]

    def leave(step):
        near_at, far_at = spots(step)
        return [
            pltpu.make_async_copy(a.at[:, near_at], b.at[:, far_at], out_sem.at[j, step])
            for j, (a, b) in enumerate(out)
        ] + [
            pltpu.make_async_copy(
                turned_ref.at[near_at], turned_hbm.at[far_at], out_sem.at[len(out), step]
            )
        ]

    begin(arrive, count // hp, 1)
    cum_copy.wait()
    cum_t_ref[...] = turn(cum_ref[...])

    def body(step, first):
        next_piece(arrive, step, count // hp, 1)
        cols = columns(cum_t_ref, start + first)
        growth = jnp.exp(cols)
        tail = jnp.exp(cols[-1:, :] - cols)
        for i in range(hp):
            lanes = lanes_of(first + i)
            qd = (q_ref[:, lanes].astype(F32) * growth[:, i : i + 1]).astype(BF16)
            qd_ref[:, lanes] = qd
            turned_ref[lanes, :] = qd.T
            tail_i = jnp.broadcast_to(tail[:, i : i + 1], (tail.shape[0], DH))
            kd_ref[:, lanes] = (k_ref[:, lanes].astype(F32) * tail_i).astype(BF16)
            vd_ref[:, lanes] = (v_ref[:, lanes].astype(F32) * tail_i).astype(BF16)
            state = None
            base = jnp.zeros((1, 1), F32)
            for j in range(n):
                at = slice(j * CHUNK, (j + 1) * CHUNK)
                col = cols[at, i : i + 1]
                end = col[CHUNK - 1 :, :]
                row = cum_ref[pl.ds(start + first + i, 1), at]
                q, k, v = q_ref[at, lanes], k_ref[at, lanes], v_ref[at, lanes]
                a = attend(q, k, v, col, row)
                if j > 0:
                    a = a + jnp.exp(col - base) * dot(q, state.astype(BF16), 1, 0)
                out_ref[at, lanes] = a.astype(BF16)
                if j < n - 1:
                    new = dot(late(k, row, end), v, 1, 0)
                    state = new if state is None else state * jnp.exp(end - base) + new
                base = end
        for copy in leave(step):
            copy.start()

    over_heads(count, hp, body)
    for step in range(count // hp):
        for copy in leave(step):
            copy.wait()


def fetch_kernel(*refs):
    n = (len(refs) - 2) // 2
    sems = refs[-1]
    copies = [pltpu.make_async_copy(refs[i], refs[n + 1 + i], sems.at[i]) for i in range(n)]
    for copy in copies:
        copy.start()
    for copy in copies:
        copy.wait()


def sums_kernel(
    hp, core_ref, mine_ref, theirs_ref, gain_ref, q_ref, sibling_ref, g_in, a_in, cum_in, turned_in,
    after_ref, att_ref, g_ref, turned_ref, sum_ref, cum_ref, s_hbm,
    sq, cross, s_ref, a_ref, g_sem, a_sem, turned_sem, s_sem, cum_sem,
):
    heads = s_ref.shape[0]
    for i in range(heads // hp):
        copy_piece(g_in, g_ref, g_sem, i, hp).start()
        copy_piece(a_in, a_ref, a_sem, i, hp).start()
    core = core_ref[0]

    def assemble(h, carry):
        for half in range(2):
            s_ref[h, 64 * half : 64 * half + 64] = half_state(
                core, 2 * h + half, mine_ref, theirs_ref, sibling_ref, 1, 64
            )
        return carry

    cum_copy = pltpu.make_async_copy(cum_in, cum_ref, cum_sem)
    cum_copy.start()
    turned = pltpu.make_async_copy(turned_in, turned_ref, turned_sem)
    turned.start()
    lax.fori_loop(0, heads, assemble, 0)
    leave = pltpu.make_async_copy(s_ref, s_hbm, s_sem)
    leave.start()
    sq[...] = jnp.zeros_like(sq)
    cross[...] = jnp.zeros_like(cross)

    def body(step, first):
        copy_piece(g_in, g_ref, g_sem, step, hp).wait()
        copy_piece(a_in, a_ref, a_sem, step, hp).wait()
        sq_sum, cross_sum = sq[...], cross[...]
        for i in range(0, hp, 2):
            h = first + i
            lanes = lanes_of(h, 2)
            both = pair(s_ref[h].astype(BF16), s_ref[h + 1].astype(BF16))
            att = a_ref[:, lanes].astype(F32) + dot(q_ref[:, lanes], both, 1, 0)
            att_ref[:, lanes] = att
            gg = g_ref[:, lanes].astype(F32) * gain_ref[:, lanes]
            square, product = att * att, gg * att
            sq_sum = sq_sum + (square[:, :DH] + square[:, DH:])
            cross_sum = cross_sum + (product[:, :DH] + product[:, DH:])
        sq[...] = sq_sum
        cross[...] = cross_sum

    over_heads(heads, hp, body)
    a = jnp.sum(sq[...].T, axis=0, keepdims=True)
    b = jnp.sum(cross[...].T, axis=0, keepdims=True)
    which = lax.broadcasted_iota(jnp.int32, sum_ref.shape, 0)
    sum_ref[...] = jnp.where(which == 0, a, b)
    turned.wait()
    cum_copy.wait()
    leave.wait()


def grad_kernel(
    hp, cum_ref, turned_ref, g_ref, att_ref, gain_ref, s0, s1, s2, s3, state_ref, out_hbm, ga_hbm,
    inv_ref, both_ref, out_ref, ga_ref, out_sem,
):
    sums = (s0[...] + s1[...]) + (s2[...] + s3[...])
    inverse = lax.rsqrt(sums[0:1] / HD + EPSILON)
    center = sums[1:2] * inverse / HD
    both = inverse * inverse * center
    length = both.shape[1]
    inv_ref[...] = jnp.broadcast_to(inverse, (128, length)).T
    both_ref[...] = jnp.broadcast_to(both, (128, length)).T
    heads = state_ref.shape[0] // 2
    which = lax.broadcasted_iota(jnp.int32, (8, DH), 0)

    def leave(step):
        return (
            copy_piece(out_ref, out_hbm, out_sem.at[0], step, hp),
            copy_piece(ga_ref, ga_hbm, out_sem.at[1], step, hp),
        )

    def body(step, first):
        inverse, both = inv_ref[...], both_ref[...]
        for i in range(hp):
            lanes = lanes_of(first + i)
            att = att_ref[:, lanes]
            gain = gain_ref[:, lanes]
            scaled = g_ref[:, lanes].astype(F32) * inverse
            ga = (scaled * gain - both * att).astype(BF16)
            ga_ref[:, lanes] = ga
            out_ref[:, lanes] = (att * inverse * gain).astype(BF16)
            gain_part = jnp.sum(scaled * att, axis=0, keepdims=True)
            turned = turned_ref[pl.ds(pl.multiple_of((first + i) * DH, DH), DH), :]
            decay = jnp.exp(cum_ref[pl.ds(first + i, 1), :][:, -1:])
            extra = jnp.where(which == 0, gain_part, decay)
            send_state(state_ref, first + i, dot(turned, ga, 1, 0), extra)
        for copy in leave(step):
            copy.start()

    over_heads(heads, hp, body)
    for step in range(heads // hp):
        for copy in leave(step):
            copy.wait()


def backward_kernel(
    hp, n, start, cum_in, s_in, q_in, k_in, v_in, ga_in, after_ref, *refs
):
    gq_hbm, gk_hbm, gv_hbm, mark_ref = refs[-18:-14]
    q_ref, k_ref, v_ref, ga_ref, gq_ref, gk_ref, gv_ref = refs[-14:-7]
    cum_ref, s_ref, cum_t_ref, cum_sem, s_sem, in_sem, out_sem = refs[-7:]
    cum_copy = pltpu.make_async_copy(cum_in, cum_ref, cum_sem)
    cum_copy.start()
    mark_ref[...] = jnp.zeros_like(mark_ref)
    count = gk_ref.shape[1] // DH
    into = ((q_in, q_ref), (k_in, k_ref), (v_in, v_ref), (ga_in, ga_ref))
    out = ((gq_ref, gq_hbm), (gk_ref, gk_hbm), (gv_ref, gv_hbm))

    def spots(step):
        return lanes_of(step * hp, hp), lanes_of(start + step * hp, hp)

    def arrive(step):
        near_at, far_at = spots(step)
        return [
            pltpu.make_async_copy(a.at[:, far_at], b.at[:, near_at], in_sem.at[j, step])
            for j, (a, b) in enumerate(into)
        ] + [
            pltpu.make_async_copy(
                s_in.at[pl.ds(start + step * hp, hp)], s_ref.at[pl.ds(step * hp, hp)], s_sem.at[step]
            )
        ]

    def leave(step):
        near_at, far_at = spots(step)
        return [
            pltpu.make_async_copy(a.at[:, near_at], b.at[:, far_at], out_sem.at[j, step])
            for j, (a, b) in enumerate(out)
        ]

    begin(arrive, count // hp, 1)
    cum_copy.wait()
    cum_t_ref[...] = turn(cum_ref[...])

    def body(step, first):
        next_piece(arrive, step, count // hp, 1)
        cols = columns(cum_t_ref, start + first)
        for i in range(hp):
            h = start + first + i
            lanes = lanes_of(first + i)
            states = [s_ref[first + i]]
            ends = [jnp.zeros((1, 1), F32)]
            for j in range(n):
                at = slice(j * CHUNK, (j + 1) * CHUNK)
                col = cols[at, i : i + 1]
                end = col[CHUNK - 1 :, :]
                if j < n - 1:
                    row = cum_ref[pl.ds(h, 1), at]
                    kd = late(k_ref[at, lanes], row, end)
                    states.append(
                        states[-1] * jnp.exp(end - ends[-1]) + dot(kd, v_ref[at, lanes], 1, 0)
                    )
                ends.append(end)
            after = None
            for j in reversed(range(n)):
                at = slice(j * CHUNK, (j + 1) * CHUNK)
                col = cols[at, i : i + 1]
                row = cum_ref[pl.ds(h, 1), at]
                q, k, v = q_ref[at, lanes], k_ref[at, lanes], v_ref[at, lanes]
                ga = ga_ref[at, lanes]
                gq, gk, gv = attend_back(q, k, v, ga, col, row)
                gq = gq + jnp.exp(col - ends[j]) * dot(ga, states[j].astype(BF16), 1, 1)
                if after is not None:
                    tail = jnp.exp(ends[j + 1] - col)
                    low = after.astype(BF16)
                    gk = gk + tail * dot(v, low, 1, 1)
                    gv = gv + tail * dot(k, low, 1, 0)
                gq_ref[at, lanes] = gq.astype(BF16)
                gk_ref[at, lanes] = gk.astype(BF16)
                gv_ref[at, lanes] = gv.astype(BF16)
                if j > 0:
                    qd = (q.T.astype(F32) * jnp.exp(row - ends[j])).astype(BF16)
                    new = dot(qd, ga, 1, 0)
                    after = new if after is None else after * jnp.exp(ends[j + 1] - ends[j]) + new
        for copy in leave(step):
            copy.start()

    over_heads(count, hp, body)
    for step in range(count // hp):
        for copy in leave(step):
            copy.wait()


def final_kernel(
    hp, core_ref, mine_ref, theirs_ref, k_ref, v_ref, sibling_ref, gk_in, gv_in, after_ref,
    gk_hbm, gv_hbm, gain_ref, gk_ref, gv_ref, in_sem, out_sem,
):
    core = core_ref[0]
    into = ((gk_in, gk_ref), (gv_in, gv_ref))
    heads = sibling_ref.shape[0] // 2

    def arrive(step):
        return [copy_piece(a, b, in_sem.at[j], step, hp) for j, (a, b) in enumerate(into)]

    def leave(step):
        return (
            copy_piece(gk_ref, gk_hbm, out_sem.at[0], step, hp),
            copy_piece(gv_ref, gv_hbm, out_sem.at[1], step, hp),
        )

    for i in range(heads // hp):
        for copy in arrive(i):
            copy.start()

    def body(step, first):
        for copy in arrive(step):
            copy.wait()
        for i in range(0, hp, 2):
            h = first + i
            lanes = lanes_of(h, 2)
            states = []
            for j in (h, h + 1):
                halves = [
                    half_state(core, m, mine_ref, theirs_ref, sibling_ref, 0, 65)
                    for m in (2 * j, 2 * j + 1)
                ]
                n = mine_ref.shape[0]
                own = (2 * j >= core * n) & (2 * j < core * n + n)
                at = lax.rem(2 * j, n)
                gain_ref[:, lanes_of(j)] = jnp.where(
                    own, mine_ref[at, 64:65], theirs_ref[at, 64:65]
                )
                states.append(jnp.concatenate(halves, axis=0).astype(BF16))
            both = pair(*states)
            gk_ref[:, lanes] = (
                gk_ref[:, lanes].astype(F32) + dot(v_ref[:, lanes], both, 1, 1)
            ).astype(BF16)
            gv_ref[:, lanes] = (
                gv_ref[:, lanes].astype(F32) + dot(k_ref[:, lanes], both, 1, 0)
            ).astype(BF16)
        for copy in leave(step):
            copy.start()

    over_heads(heads, hp, body)
    for step in range(heads // hp):
        for copy in leave(step):
            copy.wait()


def by_core(core, mine, theirs):
    return jnp.where(core == 0, mine, theirs), jnp.where(core == 0, theirs, mine)


def combine_forward_kernel(core_ref, mine_ref, theirs_ref, out_ref):
    core = core_ref[0]
    n = out_ref.shape[0]
    for i in range(n):
        at = core * n + i
        first, second = by_core(core, mine_ref[at], theirs_ref[at])
        decay = second[64:65]
        out_ref[i, 0:64] = first[0:64] * decay + second[0:64]
        out_ref[i, 64:72] = first[64:72] * second[64:72]


def combine_backward_kernel(core_ref, mine_ref, theirs_ref, out_ref):
    core = core_ref[0]
    n = out_ref.shape[0]
    which = lax.broadcasted_iota(jnp.int32, (8, DH), 0)
    for i in range(n):
        at = core * n + i
        first, second = by_core(core, mine_ref[at], theirs_ref[at])
        out_ref[i, 0:64] = second[0:64] * first[65:66] + first[0:64]
        out_ref[i, 64:72] = jnp.where(
            which == 0, first[64:72] + second[64:72], first[64:72] * second[64:72]
        )


def scan_forward_kernel(x_ref, mark_ref, out_ref):
    n = x_ref.shape[0]
    state = jnp.zeros((64, 128), F32)
    for j in range(n):
        out_ref[j] = state
        if j < n - 1:
            state = state * x_ref[j, 64:65] + x_ref[j, 0:64]


def scan_backward_kernel(x_ref, mark_ref, out_ref):
    n = x_ref.shape[0]
    state = jnp.zeros((64, 128), F32)
    gain = jnp.zeros((8, 128), F32)
    for j in reversed(range(n)):
        out_ref[j, 0:64] = state
        state = state * x_ref[j, 65:66] + x_ref[j, 0:64]
        gain = gain + x_ref[j, 64:72]
    for j in range(n):
        out_ref[j, 64:72] = gain


def half_state(core, m, mine_ref, theirs_ref, sibling_ref, last, row):
    n = mine_ref.shape[0]
    here = core * n
    own = (m >= here) & (m < here + n)
    at = lax.rem(m, n)
    value = jnp.where(own, mine_ref[at, 0:64], theirs_ref[at, 0:64])
    beside = sibling_ref[m]
    return jnp.where(core == last, value * beside[row : row + 1] + beside[0:64], value)


def cost(flops, moved, exps=0):
    return pl.CostEstimate(flops=int(flops), bytes_accessed=int(moved), transcendentals=int(exps))


def far(x):
    return pltpu.with_memory_space_constraint(x, pltpu.HBM)


def near(x):
    return pltpu.with_memory_space_constraint(x, pltpu.VMEM)


def exchange(x, axes):
    return lax.all_to_all(x, axes, split_axis=0, concat_axis=0, tiled=True)


def beside(x):
    return lax.ppermute(x, SEQ[2], [(0, 1), (1, 0)])


def other_heads(sums):
    groups = lax.axis_size("head")
    return [
        lax.ppermute(sums, "head", [(i, (i + shift) % groups) for i in range(groups)])
        for shift in range(1, groups)
    ]


def on_device(queries, key_rows, value_rows, log_decay, norm_gain, grad_out):
    tokens, width = queries.shape
    heads = width // DH
    devices = 2 * heads
    chunks = tokens // CHUNK
    gain = norm_gain[None, :]
    rows = (tokens, width)
    flat = pltpu.HBM(rows, BF16)
    kept = pltpu.VMEM(rows, BF16)
    sent = pltpu.HBM((devices, 72, DH), F32)
    joined = pltpu.HBM((devices // 2, 72, DH), F32)
    core = lax.axis_index(SEQ[2])[None].astype(jnp.int32)
    scalar = pl.BlockSpec(memory_space=pltpu.SMEM)
    here = pl.BlockSpec(memory_space=pltpu.VMEM)
    there = pl.BlockSpec(memory_space=pl.ANY)
    settings = pltpu.CompilerParams(vmem_limit_bytes=LIMIT)
    queries, key_rows, value_rows, grad_out = map(far, (queries, key_rows, value_rows, grad_out))

    def sems(*n):
        return pltpu.SemaphoreType.DMA(n)

    hp = 4
    local, cum = pl.pallas_call(
        functools.partial(local_kernel, hp),
        in_specs=[here, there, there],
        out_specs=[here] * 2,
        out_shape=[pltpu.VMEM(sent.shape, F32), pltpu.HBM((heads, tokens), F32)],
        scratch_shapes=[kept] * 2 + [sems(heads // hp)] * 2,
        compiler_params=settings,
        name="local_state",
    )(far(log_decay), key_rows, value_rows)
    cum = far(cum)

    mark_shape = pltpu.HBM((8, 128), F32)
    cum_t_shape = pltpu.VMEM((tokens, 128), F32)
    cum_shape = pltpu.VMEM((heads, tokens), F32)
    one_sem = pltpu.SemaphoreType.DMA

    def forward_part(start, count, after, ready):
        hp = 2
        part = pltpu.VMEM((tokens, count * DH), BF16)
        part_t = pltpu.VMEM((count * DH, tokens), BF16)
        *ready, mark = pl.pallas_call(
            functools.partial(forward_kernel, hp, chunks, start),
            in_specs=[there] * (5 + len(ready)),
            out_specs=[there] * 5 + [here],
            out_shape=[flat, pltpu.HBM((width, tokens), BF16), flat, flat, flat, mark_shape],
            scratch_shapes=[part] * 4
            + [part_t]
            + [part] * 3
            + [cum_shape, cum_t_shape, one_sem, sems(3, count // hp), sems(5, count // hp)],
            input_output_aliases={5 + i: i for i in range(len(ready))},
            compiler_params=settings,
            cost_estimate=cost(8e9, 13e6, 3e6),
            name="forward_intra",
        )(cum, queries, key_rows, value_rows, far(after), *map(far, ready))
        return ready, far(mark)

    def backward_part(start, count, after, ready):
        hp = 2
        part = pltpu.VMEM((tokens, count * DH), BF16)
        *ready, mark = pl.pallas_call(
            functools.partial(backward_kernel, hp, chunks, start),
            in_specs=[there] * (7 + len(ready)),
            out_specs=[there] * 3 + [here],
            out_shape=[flat] * 3 + [mark_shape],
            scratch_shapes=[part] * 7
            + [cum_shape, pltpu.VMEM((count, DH, DH), F32), cum_t_shape, one_sem]
            + [sems(count // hp), sems(4, count // hp), sems(3, count // hp)],
            input_output_aliases={7 + i: i for i in range(len(ready))},
            compiler_params=settings,
            cost_estimate=cost(10e9, 15e6, 2e6),
            name="backward_intra",
        )(
            cum, far(state_in), queries, key_rows, value_rows, far(grad_attended), far(after),
            *map(far, ready),
        )
        return ready, far(mark)

    def travel(chip, axes, scan, part, counts):
        got = exchange(chip, axes)
        ready, mark = part(0, counts[0], chip, [])
        passed = scan(got, mark)
        edge = exchange(passed, axes)
        ready, mark = part(counts[0], counts[1], passed, ready)
        edge, last = lax.optimization_barrier((edge, mark))
        return edge, far(last), ready

    sibling = beside(near(local))
    chip = pl.pallas_call(
        combine_forward_kernel,
        in_specs=[scalar, here, here],
        out_specs=here,
        out_shape=joined,
        compiler_params=settings,
        name="combine_forward",
    )(core, near(local), near(sibling))

    def scan_forward(got, mark):
        return pl.pallas_call(
            scan_forward_kernel,
            in_specs=[here, there],
            out_specs=here,
            out_shape=pltpu.HBM((devices // 2, 64, DH), F32),
            compiler_params=settings,
            name="scan_forward",
        )(got, mark)

    chip_state, last, ready = travel(chip, SEQ[:2], scan_forward, forward_part, FORWARD_CUTS)
    sibling_state = beside(chip_state)
    attended_local, turned, grown, faded_k, faded_v = map(far, ready)

    def fetch(after, *arrays):
        return pl.pallas_call(
            fetch_kernel,
            in_specs=[there] * (len(arrays) + 1),
            out_specs=[here] * len(arrays),
            out_shape=[pltpu.VMEM(x.shape, x.dtype) for x in arrays],
            scratch_shapes=[sems(len(arrays))],
            compiler_params=settings,
            cost_estimate=cost(1e9, 19e6),
            name="fetch_rows",
        )(*map(far, arrays), after)

    grown, sibling_here = fetch(chip_state, grown, sibling)

    hp = 4
    attended, grads, turned, sums, cum_here, state_in = pl.pallas_call(
        functools.partial(sums_kernel, hp),
        in_specs=[scalar] + [here] * 5 + [there] * 5,
        out_specs=[here] * 5 + [there],
        out_shape=[
            pltpu.VMEM(rows, F32),
            kept,
            pltpu.VMEM((width, tokens), BF16),
            pltpu.VMEM((8, tokens), F32),
            pltpu.VMEM((heads, tokens), F32),
            pltpu.HBM((heads, DH, DH), F32),
        ],
        scratch_shapes=[pltpu.VMEM((tokens, 128), F32)] * 2
        + [pltpu.VMEM((heads, DH, DH), F32), kept]
        + [sems(heads // hp)] * 2
        + [pltpu.SemaphoreType.DMA] * 3,
        compiler_params=settings,
        name="row_sums",
    )(
        core, chip_state, near(sibling_state), gain, near(grown),
        near(sibling_here), grad_out, attended_local, cum, turned, last,
    )

    hp = 4
    others = other_heads(sums)
    sent_grad, output, grad_attended = pl.pallas_call(
        functools.partial(grad_kernel, hp),
        in_specs=[here] * 9,
        out_specs=[here] + [there] * 2,
        out_shape=[pltpu.VMEM(sent.shape, F32), flat, flat],
        scratch_shapes=[pltpu.VMEM((tokens, 128), F32)] * 2 + [kept] * 2 + [sems(2, heads // hp)],
        compiler_params=settings,
        name="grad_state",
    )(near(cum_here), near(turned), near(grads), near(attended), gain, *map(near, (sums, *others)))

    def scan_backward(got_grad, mark):
        return pl.pallas_call(
            scan_backward_kernel,
            in_specs=[here, there],
            out_specs=here,
            out_shape=joined,
            compiler_params=settings,
            name="scan_backward",
        )(got_grad, mark)

    sibling_grad = beside(near(sent_grad))
    chip_grad = pl.pallas_call(
        combine_backward_kernel,
        in_specs=[scalar, here, here],
        out_specs=here,
        out_shape=joined,
        compiler_params=settings,
        name="combine_backward",
    )(core, near(sent_grad), near(sibling_grad))
    chip_after, last_grad, ready = travel(
        chip_grad, SEQ[:2], scan_backward, backward_part, BACKWARD_CUTS
    )
    sibling_after = beside(chip_after)
    grad_q, part_k, part_v = ready

    faded_k, faded_v, sibling_here = fetch(chip_after, faded_k, faded_v, sibling_grad)

    hp = 4
    grad_k, grad_v, grad_gain = pl.pallas_call(
        functools.partial(final_kernel, hp),
        in_specs=[scalar] + [here] * 5 + [there] * 3,
        out_specs=[there] * 2 + [here],
        out_shape=[flat] * 2 + [jax.ShapeDtypeStruct((1, width), F32)],
        scratch_shapes=[kept] * 2 + [sems(2, heads // hp), sems(2, heads // hp)],
        compiler_params=settings,
        name="final_grads",
    )(
        core, chip_after, near(sibling_after), near(faded_k), near(faded_v), near(sibling_here),
        far(part_k), far(part_v), last_grad,
    )
    return output, grad_q, grad_k, grad_v, grad_gain.reshape(width)


def solution(mesh):
    split = Mesh(
        mesh.devices.reshape(4, 4, 2, mesh.shape["head"]), ("seq_0", "seq_1", "seq_2", "head")
    )
    placed = (
        P(SEQ, "head"),
        P(SEQ, "head"),
        P(SEQ, "head"),
        P("head", SEQ),
        P("head"),
        P(SEQ, "head"),
    )
    return jax.shard_map(
        on_device,
        mesh=split,
        in_specs=placed,
        out_specs=(P(SEQ, "head"), P(SEQ, "head"), P(SEQ, "head"), P(SEQ, "head"), P("head")),
        check_vma=False,
    )
```
